32 devices in a mesh: dp: 4 (over x, y), tp: 8 (over z, core).
Axes of the slice: x: 2, y: 2, z: 4, core: 2. Of those that a mesh axis runs over, the one named last changes fastest.
Arguments:
- x: bfloat16 [13312, 2560], P(('dp', 'tp')), parts along dimension 0
- dy: bfloat16 [13312, 2560], P(('dp', 'tp')), parts along dimension 0
- pre: bfloat16 [13312, 10240], P('dp', 'tp'), parts along dimension 0
- w_in: bfloat16 [2560, 10240], P(None, 'tp')
- w_down: bfloat16 [10240, 2560], P('tp')
Outputs:
- output 1: bfloat16 [13312, 2560], P(('dp', 'tp')), parts along dimension 0
- output 2: bfloat16 [10240, 10240], P('dp', 'tp'), parts along dimension 0
- output 3: bfloat16 [40960, 2560], P(('dp', 'tp')), parts along dimension 0
There are 4 independent parts. The reference program is written for one: setup_inputs(seed, part) draws one part's arguments, and reference() takes and returns one part's arrays. A program takes and returns all parts, laid end to end along the dimension named above; an argument that names none is the same for every part.
All inputs are finite; a program needn't handle non-finite values.
Results may differ from the reference program's by a relative error of at most 0.012.
Values are sent between devices in bfloat16 or wider.
A program may use at most 2 GiB of HBM per device.

```python
import jax
import jax.numpy as jnp

ROWS = 3328
D = 2560
FF = 10240


def act(pre):
    return jax.nn.gelu(pre)


def setup_inputs(seed: int = 0, part: int = 0) -> dict:
    kx, ky, ka, ki, kd = jax.random.split(jax.random.key(seed), 5)
    kx, ky, ka = (jax.random.fold_in(k, part) for k in (kx, ky, ka))
    drawn = {
        "x": jax.random.normal(kx, (ROWS, D), jnp.float32),
        "dy": jax.random.normal(ky, (ROWS, D), jnp.float32),
        "pre": jax.random.normal(ka, (ROWS, FF), jnp.float32),
        "w_in": jax.random.normal(ki, (D, FF), jnp.float32) * D**-0.5,
        "w_down": jax.random.normal(kd, (FF, D), jnp.float32) * FF**-0.5,
    }
    return {k: v.astype(jnp.bfloat16) for k, v in drawn.items()}


def reference(x, dy, pre, w_in, w_down):
    hidden, back = jax.vjp(act, pre.astype(jnp.float32))
    d_hidden = jnp.dot(dy, w_down.T, preferred_element_type=jnp.float32)
    d_pre = back(d_hidden)[0].astype(jnp.bfloat16)
    dx = jnp.dot(d_pre, w_in.T, preferred_element_type=jnp.float32)
    dw_in = jnp.dot(x.T, d_pre, preferred_element_type=jnp.float32)
    dw_down = jnp.dot(hidden.astype(jnp.bfloat16).T, dy, preferred_element_type=jnp.float32)
    return tuple(g.astype(jnp.bfloat16) for g in (dx, dw_in, dw_down))
```

```python
import functools

import jax
import jax.numpy as jnp
from jax import lax
from jax.experimental import pallas as pl
from jax.experimental.pallas import tpu as pltpu
from jax.sharding import PartitionSpec as P

Z = 4
NT = (((1,), (1,)), ((), ()))
TN = (((0,), (0,)), ((), ()))
F32, BF16 = jnp.float32, jnp.bfloat16
K0 = 0.7978845608028654
K1 = 0.044715
TILE = 256


def gelu_and_slope(p):
    p2 = p * p
    t = jnp.tanh(K0 * (p + K1 * (p * p2)))
    cdf = 0.5 * (1.0 + t)
    slope = cdf + (0.5 * p) * (1.0 - t * t) * (K0 * (1.0 + (3.0 * K1) * p2))
    return p * cdf, slope


def line_kernel(
    x_ref, dy_ref, pre_ref, wi_ref, wd_ref,
    xg, dyg, dpre_o, dwd_o, base_o, last_o, rin, pin, rout,
    wi, wd, acc, dp, dyb, preb, hid, pxb, pv, rv, sb, bb,
    ssem, rsem, ps, pr, pxs, pxr, rs_s, rs_r, lsem,
):
    B, D = dy_ref.shape
    H = B // 2
    F = wd_ref.shape[0]
    PAD = dyb.shape[0]
    tp = lax.axis_index("tp")
    z, c = tp // 2, tp % 2
    partner = z * 2 + (1 - c)
    arrs, gathered = (dy_ref, x_ref), (dyg, xg)
    sign = (1, -1)
    place = (z, Z - 1 - z)
    ahead = tuple(jnp.clip(tp + 2 * s, 0, 2 * Z - 1) for s in sign)

    def remote(src, dst, send, recv, to):
        return pltpu.make_async_remote_copy(
            src_ref=src, dst_ref=dst, send_sem=send, recv_sem=recv,
            device_id={"tp": to}, device_id_type=pl.DeviceIdType.MESH,
        )

    def local(src, dst, i):
        return pltpu.make_async_copy(src, dst, lsem.at[i])

    def sync(src, dst, i):
        cp = local(src, dst, i)
        cp.start()
        cp.wait()

    def rows_of(chip, core, h):
        return pl.ds(pl.multiple_of((chip * 2 + core) * B + h * H, 16), H)

    def block_of(chip, core):
        return pl.ds(pl.multiple_of((chip * 2 + core) * B, 32), B)

    def half(h):
        return pl.ds(pl.multiple_of(h * H, 16), H)

    barrier = pltpu.get_barrier_semaphore()
    pl.semaphore_signal(barrier, inc=1, device_id={"tp": partner}, device_id_type=pl.DeviceIdType.MESH)
    for d in (0, 1):
        @pl.when(place[d] < Z - 1)
        def _():
            pl.semaphore_signal(barrier, inc=1, device_id={"tp": ahead[d]}, device_id_type=pl.DeviceIdType.MESH)
    pl.semaphore_wait(barrier, jnp.where((z > 0) & (z < Z - 1), 3, 2))

    def own_send(d, a, h):
        return remote(arrs[a].at[half(h)], gathered[a].at[rows_of(z, c, h)],
                      ssem.at[d, a, 0, h], rsem.at[d, a, 0, h], ahead[d])

    def line_send(d, a, s, h):
        r = rows_of(z - sign[d] * s, c, h)
        return remote(gathered[a].at[r], gathered[a].at[r],
                      ssem.at[d, a, s, h], rsem.at[d, a, s, h], ahead[d])

    def line_arrival(d, a, s, h):
        r = rows_of(z - sign[d] * s, c, h)
        return remote(gathered[a].at[r], gathered[a].at[r],
                      ssem.at[d, a, 0, h], rsem.at[d, a, s - 1, h], ahead[d])

    def own_to_partner(a, h):
        return remote(arrs[a].at[half(h)], gathered[a].at[rows_of(z, c, h)],
                      ps.at[a, z, h], pr.at[a, z, h], partner)

    def to_partner(a, chip, h):
        r = rows_of(chip, c, h)
        return remote(gathered[a].at[r], gathered[a].at[r],
                      ps.at[a, chip, h], pr.at[a, chip, h], partner)

    def from_partner(a, chip, h):
        r = rows_of(chip, 1 - c, h)
        return remote(gathered[a].at[r], gathered[a].at[r],
                      ps.at[a, chip, h], pr.at[a, chip, h], partner)

    for h in (0, 1):
        for d in (0, 1):
            @pl.when(place[d] < Z - 1)
            def _():
                own_send(d, 0, h).start()
    for h in (0, 1):
        own_to_partner(0, h).start()
    local(wd_ref, wd, 6).start()
    local(wi_ref, wi, 7).start()
    for h in (0, 1):
        own_to_partner(1, h).start()

    dyb[pl.ds(B, PAD - B), :] = jnp.zeros((PAD - B, D), BF16)
    hid[pl.ds(B, PAD - B), :] = jnp.zeros((PAD - B, F), BF16)

    def zero(i, _):
        acc[pl.ds(pl.multiple_of(i * 64, 64), 64), :] = jnp.zeros((64, D), F32)
        return 0

    lax.fori_loop(0, F // 64, zero, 0)
    local(wd_ref, wd, 6).wait()
    local(wi_ref, wi, 7).wait()

    def arrive(d, a, s, h):
        line_arrival(d, a, s, h).wait_recv()

        @pl.when(place[d] < Z - 1)
        def _():
            line_send(d, a, s, h).start()
        to_partner(a, z - sign[d] * s, h).start()

    def chip_at(k):
        outer = (z == 0) | (z == Z - 1)
        o = jnp.where(outer, k, jnp.where(k < 2, 1 - k, k))
        return jnp.where(z < 2, o, Z - 1 - o)

    def px_send(chip, k):
        return remote(pxb, pin.at[chip], pxs.at[k], pxr.at[chip], partner)

    def cols(n, width=TILE):
        return pl.ds(pl.multiple_of(n * width, width), width)

    def slot(t, _):
        s, h = (t + 1) // 2, (t + 1) % 2
        for d in (0, 1):
            q = place[d]

            @pl.when((t >= 1) & (s <= q))
            def _():
                arrive(d, 0, s, h)

            @pl.when((t >= 1) & (s > q) & (s <= 2 * q))
            def _():
                arrive(d, 1, s - q, h)

            @pl.when((t == 2 * q) & (q < Z - 1))
            def _():
                for hh in (0, 1):
                    own_send(d, 1, hh).start()

        def rs(j, _):
            outer = (z == 0) | (z == Z - 1)
            u0, u1 = jnp.maximum(t - 4, 0), jnp.maximum(t - 7, 0)
            k = jnp.where(outer, (u0 // 2 + 1) % 4, jnp.where(j == 0, (u1 // 2 + 2) % 4, 1))
            b = jnp.where(z < 2, k, Z - 1 - k)
            hh = jnp.where(outer, u0 % 2, jnp.where(j == 0, u1 % 2, (t + 1) % 2))
            first = jnp.where(outer, 4, jnp.where(j == 0, 7, 9))
            end = jnp.where(outer, jnp.where(j == 0, 12, 0), jnp.where(j == 0, 13, 11))

            @pl.when((t >= first) & (t < end))
            def _():
                inner = (z > 0) & (z < Z - 1)
                has = (inner & (b >= z), inner & (b <= z))

                @pl.when(hh == 0)
                def _():
                    remote(pxb, pin.at[b], pxs.at[0], pxr.at[b], partner).wait_recv()
                local(pin.at[b, half(hh)], pv, 0).start()
                for d in (0, 1):
                    @pl.when(has[d])
                    def _():
                        remote(rin.at[d, b, half(hh)], rin.at[d, b, half(hh)],
                               rs_s.at[b, hh], rs_r.at[d, b, hh], partner).wait_recv()
                        local(rin.at[d, b, half(hh)], rv.at[d], 1 + d).start()

                    @pl.when(jnp.logical_not(has[d]))
                    def _():
                        rv[d] = jnp.zeros(rv.shape[1:], BF16)
                local(pin.at[b, half(hh)], pv, 0).wait()
                for d in (0, 1):
                    @pl.when(has[d])
                    def _():
                        local(rin.at[d, b, half(hh)], rv.at[d], 1 + d).wait()

                def tile(n, _):
                    cs = cols(n)
                    g = lax.dot_general(dp[rows_of(b, c, hh), :], wi[cs, :], NT, preferred_element_type=F32)
                    g = g + pv[:, cs].astype(F32)
                    g = g + (rv[0, :, cs].astype(F32) + rv[1, :, cs].astype(F32))
                    bb[:, cs] = g
                    sb[:, cs] = g.astype(BF16)
                    return 0

                lax.fori_loop(0, D // TILE, tile, 0)
                to_last = ((z == 1) & (b == 0)) | ((z == Z - 2) & (b == Z - 1))

                @pl.when(b == z)
                def _():
                    sync(bb, base_o.at[half(hh)], 3)

                @pl.when(to_last)
                def _():
                    sync(sb, last_o.at[half(hh)], 3)

                @pl.when((b != z) & jnp.logical_not(to_last))
                def _():
                    sync(sb, rout.at[b, half(hh)], 3)
                    for d in (0, 1):
                        @pl.when((b > z) if d == 0 else (b < z))
                        def _():
                            r_send(d, b, hh).start()
            return 0

        def r_send(d, b, hh):
            return remote(rout.at[b, half(hh)], rin.at[d, b, half(hh)],
                          rs_s.at[b, hh], rs_r.at[d, b, hh], ahead[d])

        lax.fori_loop(0, 2, rs, 0)

        @pl.when(t < 8)
        def _():
            k = t // 2
            chip = chip_at(k)
            odd = t % 2
            core = jnp.where(odd == 0, c, 1 - c)
            blk = block_of(chip, core)
            local(pre_ref.at[blk], preb, 0).start()

            @pl.when(odd == 1)
            def _():
                for hh in (0, 1):
                    from_partner(0, chip, hh).wait_recv()

            @pl.when(t == 0)
            def _():
                sync(dy_ref, dyb.at[pl.ds(0, B)], 1)

            @pl.when(t > 0)
            def _():
                sync(dyg.at[blk], dyb.at[pl.ds(0, B)], 1)
            local(pre_ref.at[blk], preb, 0).wait()

            def t1(n, _):
                cs = cols(n)
                g = lax.dot_general(dyb[pl.ds(0, B), :], wd[cs, :], NT, preferred_element_type=F32)
                hidden, slope = gelu_and_slope(preb[:, cs].astype(F32))
                hid[pl.ds(0, B), cs] = hidden.astype(BF16)
                dp[blk, cs] = (g * slope).astype(BF16)
                return 0

            lax.fori_loop(0, F // TILE, t1, 0)

            @pl.when(odd == 1)
            def _():
                @pl.when(k > 0)
                def _():
                    px_send(chip, k - 1).wait_send()

                def px(n, _):
                    cs = cols(n)
                    g = lax.dot_general(dp[blk, :], wi[cs, :], NT, preferred_element_type=F32)
                    pxb[:, cs] = g.astype(BF16)
                    return 0

                lax.fori_loop(0, D // TILE, px, 0)
                px_send(chip, k).start()

            def t2(m, _):
                ms = cols(m)
                acc[ms, :] += lax.dot_general(hid[:, ms], dyb[...], TN, preferred_element_type=F32)
                return 0

            lax.fori_loop(0, F // TILE, t2, 0)

        @pl.when(t == 8)
        def _():
            local(dp, dpre_o, 4).start()
            sync(x_ref, dyb.at[pl.ds(0, B)], 1)
            sync(dyb.at[pl.ds(0, B)], xg.at[block_of(z, c)], 1)

            def flush(m, _):
                ms = cols(m)
                dyb[pl.ds(0, TILE), :] = acc[ms, :].astype(BF16)
                sync(dyb.at[pl.ds(0, TILE)], dwd_o.at[ms], 1)
                return 0

            lax.fori_loop(0, F // TILE, flush, 0)
        return 0

    lax.fori_loop(0, 13, slot, 0)

    local(dp, dpre_o, 4).wait()
    px_send(0, 3).wait_send()
    for chip in range(Z):
        for h in (0, 1):
            for a in (0, 1):
                to_partner(a, chip, h).wait_send()
            from_partner(1, chip, h).wait_recv()
            kept = ((z == 1) & (chip == 0)) | ((z == Z - 2) & (chip == Z - 1))

            @pl.when((z != chip) & jnp.logical_not(kept))
            def _():
                remote(rout.at[chip, half(h)], rin.at[0, chip, half(h)],
                       rs_s.at[chip, h], rs_r.at[0, chip, h], partner).wait_send()
    for d in (0, 1):
        for s in range(Z - 1):
            @pl.when((place[d] < Z - 1) & (s <= place[d]))
            def _():
                for a in (0, 1):
                    for h in (0, 1):
                        line_send(d, a, s, h).wait_send()


def line_step(x, dy, pre, w_in, w_down):
    B, D = dy.shape
    H = B // 2
    R, F = pre.shape
    PAD = -(-B // TILE) * TILE
    hbm = pl.BlockSpec(memory_space=pltpu.HBM)
    sds = jax.ShapeDtypeStruct
    dma = pltpu.SemaphoreType.DMA
    return pl.pallas_call(
        line_kernel,
        out_shape=[
            sds((R, D), BF16), sds((R, D), BF16), sds((R, F), BF16), sds((F, D), BF16),
            sds((B, D), F32), sds((B, D), BF16),
            sds((2, Z, B, D), BF16), sds((Z, B, D), BF16), sds((Z, B, D), BF16),
        ],
        in_specs=[hbm] * 5,
        out_specs=[hbm] * 9,
        scratch_shapes=[
            pltpu.VMEM((D, F), BF16), pltpu.VMEM((F, D), BF16), pltpu.VMEM((F, D), F32),
            pltpu.VMEM((R, F), BF16), pltpu.VMEM((PAD, D), BF16), pltpu.VMEM((B, F), BF16),
            pltpu.VMEM((PAD, F), BF16), pltpu.VMEM((B, D), BF16), pltpu.VMEM((H, D), BF16),
            pltpu.VMEM((2, H, D), BF16), pltpu.VMEM((H, D), BF16), pltpu.VMEM((H, D), F32),
            dma((2, 2, 3, 2)), dma((2, 2, 3, 2)), dma((2, Z, 2)), dma((2, Z, 2)),
            dma((Z,)), dma((Z,)), dma((Z, 2)), dma((2, Z, 2)), dma((8,)),
        ],
        compiler_params=pltpu.CompilerParams(
            collective_id=0, has_side_effects=True, vmem_limit_bytes=62 * 1024 * 1024
        ),
        cost_estimate=pl.CostEstimate(flops=6 * R * D * F, bytes_accessed=12 * R * D, transcendentals=R * F),
    )(x, dy, pre, w_in, w_down)


def dw_kernel(a_ref, b_ref, o_ref):
    o_ref[...] = lax.dot_general(a_ref[...], b_ref[...], TN, preferred_element_type=F32).astype(o_ref.dtype)


def weight_grad(a, b, width=512):
    R, D = a.shape
    F = b.shape[1]
    return pl.pallas_call(
        dw_kernel,
        grid=(D // width,),
        out_shape=jax.ShapeDtypeStruct((D, F), BF16),
        in_specs=[pl.BlockSpec((R, width), lambda i: (0, i)), pl.BlockSpec((R, F), lambda i: (0, 0))],
        out_specs=pl.BlockSpec((width, F), lambda i: (i, 0)),
        compiler_params=pltpu.CompilerParams(vmem_limit_bytes=48 * 1024 * 1024),
        cost_estimate=pl.CostEstimate(flops=2 * R * D * F, bytes_accessed=2 * (R * D + R * F + D * F), transcendentals=0),
    )(a, b)


def solution(mesh):
    def body(x, dy, pre, w_in, w_down):
        xg, _, d_pre, dw_down, base, last, _, _, _ = line_step(x, dy, pre, w_in, w_down)
        hops = [(2 + c, c) for c in (0, 1)] + [(2 * Z - 4 + c, 2 * Z - 2 + c) for c in (0, 1)]
        came = lax.ppermute(last, "tp", hops)
        dw_in = weight_grad(xg, d_pre)
        dx = (base + came.astype(F32)).astype(BF16)
        return dx, dw_in, dw_down

    rows = P(("dp", "tp"), None)
    return jax.shard_map(
        body, mesh=mesh,
        in_specs=(rows, rows, P("dp", "tp"), P(None, "tp"), P("tp", None)),
        out_specs=(rows, P("dp", "tp"), rows),
        check_vma=False,
    )
```

```python
import functools

import jax
import jax.numpy as jnp
from jax import lax
from jax.experimental import pallas as pl
from jax.experimental.pallas import tpu as pltpu
from jax.sharding import PartitionSpec as P

Z = 4
NT = (((1,), (1,)), ((), ()))
TN = (((0,), (0,)), ((), ()))
F32, BF16 = jnp.float32, jnp.bfloat16
K0 = 0.7978845608028654
K1 = 0.044715
TILE = 256


def gelu_and_slope(p):
    p2 = p * p
    t = jnp.tanh(K0 * (p + K1 * (p * p2)))
    cdf = 0.5 * (1.0 + t)
    slope = cdf + (0.5 * p) * (1.0 - t * t) * (K0 * (1.0 + (3.0 * K1) * p2))
    return p * cdf, slope


def line_kernel(
    x_ref, dy_ref, pre_ref, wi_ref, wd_ref,
    xg, dyg, dpre_o, dwd_o, part_o, base_o, late_base_o, last_o, came_o, rin, pin, rout,
    wi, wd, acc, dp, dyb, preb, hid, pxb, pv, rv, sb, bb,
    ssem, rsem, ps, pr, pxs, pxr, rs_s, rs_r, lsem,
):
    B, D = dy_ref.shape
    H = B // 2
    F = wd_ref.shape[0]
    PAD = dyb.shape[0]
    tp = lax.axis_index("tp")
    z, c = tp // 2, tp % 2
    partner = z * 2 + (1 - c)
    arrs, gathered = (dy_ref, x_ref), (dyg, xg)
    sign = (1, -1)
    place = (z, Z - 1 - z)
    ahead = tuple(jnp.clip(tp + 2 * s, 0, 2 * Z - 1) for s in sign)

    def remote(src, dst, send, recv, to):
        return pltpu.make_async_remote_copy(
            src_ref=src, dst_ref=dst, send_sem=send, recv_sem=recv,
            device_id={"tp": to}, device_id_type=pl.DeviceIdType.MESH,
        )

    def local(src, dst, i):
        return pltpu.make_async_copy(src, dst, lsem.at[i])

    def sync(src, dst, i):
        cp = local(src, dst, i)
        cp.start()
        cp.wait()

    def turn(zz, k):
        outer = (zz == 0) | (zz == Z - 1)
        o = jnp.where(outer, k, jnp.where(k < 2, 1 - k, k))
        return jnp.where(zz < 2, o, Z - 1 - o)

    def spot(a, zz, chip):
        if a == 0:
            return chip
        p = jnp.where(zz < 2, chip, Z - 1 - chip)
        outer = (zz == 0) | (zz == Z - 1)
        return jnp.where(outer, p, jnp.where(p < 2, 1 - p, p))

    def rows_of(chip, core, h):
        return pl.ds(pl.multiple_of((chip * 2 + core) * B + h * H, 16), H)

    def block_of(chip, core):
        return pl.ds(pl.multiple_of((chip * 2 + core) * B, 32), B)

    def chip_rows(chip):
        return pl.ds(pl.multiple_of(chip * 2 * B, 64), 2 * B)

    def half(h):
        return pl.ds(pl.multiple_of(h * H, 16), H)

    barrier = pltpu.get_barrier_semaphore()
    pl.semaphore_signal(barrier, inc=1, device_id={"tp": partner}, device_id_type=pl.DeviceIdType.MESH)
    for d in (0, 1):
        @pl.when(place[d] < Z - 1)
        def _():
            pl.semaphore_signal(barrier, inc=1, device_id={"tp": ahead[d]}, device_id_type=pl.DeviceIdType.MESH)
    pl.semaphore_wait(barrier, jnp.where((z > 0) & (z < Z - 1), 3, 2))

    def own_send(d, a, h):
        return remote(arrs[a].at[half(h)], gathered[a].at[rows_of(spot(a, z + sign[d], z), c, h)],
                      ssem.at[d, a, 0, h], rsem.at[d, a, 0, h], ahead[d])

    def line_send(d, a, s, h):
        chip = z - sign[d] * s
        return remote(gathered[a].at[rows_of(spot(a, z, chip), c, h)],
                      gathered[a].at[rows_of(spot(a, z + sign[d], chip), c, h)],
                      ssem.at[d, a, s, h], rsem.at[d, a, s, h], ahead[d])

    def line_arrival(d, a, s, h):
        r = rows_of(spot(a, z, z - sign[d] * s), c, h)
        return remote(gathered[a].at[r], gathered[a].at[r],
                      ssem.at[d, a, 0, h], rsem.at[d, a, s - 1, h], ahead[d])

    def own_to_partner(a, h):
        return remote(arrs[a].at[half(h)], gathered[a].at[rows_of(spot(a, z, z), c, h)],
                      ps.at[a, z, h], pr.at[a, z, h], partner)

    def to_partner(a, chip, h):
        r = rows_of(spot(a, z, chip), c, h)
        return remote(gathered[a].at[r], gathered[a].at[r],
                      ps.at[a, chip, h], pr.at[a, chip, h], partner)

    def from_partner(a, chip, h):
        r = rows_of(spot(a, z, chip), 1 - c, h)
        return remote(gathered[a].at[r], gathered[a].at[r],
                      ps.at[a, chip, h], pr.at[a, chip, h], partner)

    for h in (0, 1):
        for d in (0, 1):
            @pl.when(place[d] < Z - 1)
            def _():
                own_send(d, 0, h).start()
    for h in (0, 1):
        own_to_partner(0, h).start()
    local(wd_ref, wd, 6).start()
    local(wi_ref, wi, 7).start()
    for h in (0, 1):
        own_to_partner(1, h).start()

    dyb[pl.ds(B, PAD - B), :] = jnp.zeros((PAD - B, D), BF16)
    hid[pl.ds(B, PAD - B), :] = jnp.zeros((PAD - B, F), BF16)

    def zero(i, _):
        acc[pl.ds(pl.multiple_of(i * 64, 64), 64), :] = jnp.zeros((64, D), F32)
        return 0

    lax.fori_loop(0, F // 64, zero, 0)
    local(wd_ref, wd, 6).wait()
    local(wi_ref, wi, 7).wait()

    def arrive(d, a, s, h):
        line_arrival(d, a, s, h).wait_recv()

        @pl.when(place[d] < Z - 1)
        def _():
            line_send(d, a, s, h).start()
        to_partner(a, z - sign[d] * s, h).start()

    def px_send(chip, k):
        return remote(pxb, pin.at[chip], pxs.at[k], pxr.at[chip], partner)

    def cols(n, width=TILE):
        return pl.ds(pl.multiple_of(n * width, width), width)

    def slot(t, _):
        s, h = (t + 1) // 2, (t + 1) % 2
        for d in (0, 1):
            q = place[d]

            @pl.when((t >= 1) & (s <= q))
            def _():
                arrive(d, 0, s, h)

            @pl.when((t >= 1) & (s > q) & (s <= 2 * q))
            def _():
                arrive(d, 1, s - q, h)

            @pl.when((t == 2 * q) & (q < Z - 1))
            def _():
                for hh in (0, 1):
                    own_send(d, 1, hh).start()

        def rs(j, _):
            outer = (z == 0) | (z == Z - 1)
            u0, u1 = jnp.maximum(t - 4, 0), jnp.maximum(t - 7, 0)
            k = jnp.where(outer, (u0 // 2 + 1) % 4, jnp.where(j == 0, (u1 // 2 + 2) % 4, 1))
            b = jnp.where(z < 2, k, Z - 1 - k)
            hh = jnp.where(outer, u0 % 2, jnp.where(j == 0, u1 % 2, (t + 1) % 2))
            first = jnp.where(outer, 4, jnp.where(j == 0, 7, 9))
            end = jnp.where(outer, jnp.where(j == 0, 12, 0), jnp.where(j == 0, 13, 11))

            @pl.when((t >= first) & (t < end))
            def _():
                inner = (z > 0) & (z < Z - 1)
                has = (inner & (b >= z), inner & (b <= z))

                @pl.when(hh == 0)
                def _():
                    remote(pxb, pin.at[b], pxs.at[0], pxr.at[b], partner).wait_recv()
                local(pin.at[b, half(hh)], pv, 0).start()
                for d in (0, 1):
                    @pl.when(has[d])
                    def _():
                        remote(rin.at[d, b, half(hh)], rin.at[d, b, half(hh)],
                               rs_s.at[b, hh], rs_r.at[d, b, hh], partner).wait_recv()
                        local(rin.at[d, b, half(hh)], rv.at[d], 1 + d).start()

                    @pl.when(jnp.logical_not(has[d]))
                    def _():
                        rv[d] = jnp.zeros(rv.shape[1:], BF16)
                local(pin.at[b, half(hh)], pv, 0).wait()
                for d in (0, 1):
                    @pl.when(has[d])
                    def _():
                        local(rin.at[d, b, half(hh)], rv.at[d], 1 + d).wait()

                def tile(n, _):
                    cs = cols(n)
                    g = lax.dot_general(dp[rows_of(b, c, hh), :], wi[cs, :], NT, preferred_element_type=F32)
                    g = g + pv[:, cs].astype(F32)
                    g = g + (rv[0, :, cs].astype(F32) + rv[1, :, cs].astype(F32))
                    bb[:, cs] = g
                    sb[:, cs] = g.astype(BF16)
                    return 0

                lax.fori_loop(0, D // TILE, tile, 0)
                to_end = ((z == 1) & (b == 0)) | ((z == Z - 2) & (b == Z - 1))
                to_last = to_end & (hh == 1)

                @pl.when(b == z)
                def _():
                    @pl.when(hh == 0)
                    def _():
                        sync(bb, base_o, 3)

                    @pl.when(hh == 1)
                    def _():
                        sync(bb, late_base_o, 3)

                @pl.when(to_last)
                def _():
                    sync(sb, last_o, 3)

                @pl.when((b != z) & jnp.logical_not(to_last))
                def _():
                    sync(sb, rout.at[b, half(hh)], 3)
                    for d in (0, 1):
                        goes = (b > z) if d == 0 else (b < z)

                        @pl.when(goes & jnp.logical_not(to_end))
                        def _():
                            r_send(d, b, hh).start()

                        @pl.when(goes & to_end)
                        def _():
                            end_send(d, b).start()
            return 0

        def r_send(d, b, hh):
            return remote(rout.at[b, half(hh)], rin.at[d, b, half(hh)],
                          rs_s.at[b, hh], rs_r.at[d, b, hh], ahead[d])

        def end_send(d, b):
            return remote(rout.at[b, half(0)], came_o, rs_s.at[b, 0], rs_r.at[d, b, 0], ahead[d])

        lax.fori_loop(0, 2, rs, 0)

        @pl.when(t < 8)
        def _():
            k = t // 2
            chip = turn(z, k)
            odd = t % 2
            core = jnp.where(odd == 0, c, 1 - c)
            blk = block_of(chip, core)
            local(pre_ref.at[blk], preb, 0).start()

            @pl.when(odd == 1)
            def _():
                for hh in (0, 1):
                    from_partner(0, chip, hh).wait_recv()

            @pl.when(t == 0)
            def _():
                sync(dy_ref, dyb.at[pl.ds(0, B)], 1)

            @pl.when(t > 0)
            def _():
                sync(dyg.at[blk], dyb.at[pl.ds(0, B)], 1)
            local(pre_ref.at[blk], preb, 0).wait()

            def t1(n, _):
                cs = cols(n)
                g = lax.dot_general(dyb[pl.ds(0, B), :], wd[cs, :], NT, preferred_element_type=F32)
                hidden, slope = gelu_and_slope(preb[:, cs].astype(F32))
                hid[pl.ds(0, B), cs] = hidden.astype(BF16)
                dp[blk, cs] = (g * slope).astype(BF16)
                return 0

            lax.fori_loop(0, F // TILE, t1, 0)

            @pl.when(odd == 1)
            def _():
                @pl.when(k > 0)
                def _():
                    px_send(chip, k - 1).wait_send()

                def px(n, _):
                    cs = cols(n)
                    g = lax.dot_general(dp[blk, :], wi[cs, :], NT, preferred_element_type=F32)
                    pxb[:, cs] = g.astype(BF16)
                    return 0

                lax.fori_loop(0, D // TILE, px, 0)
                px_send(chip, k).start()

            def t2(m, _):
                ms = cols(m)
                acc[ms, :] += lax.dot_general(hid[:, ms], dyb[...], TN, preferred_element_type=F32)
                return 0

            lax.fori_loop(0, F // TILE, t2, 0)

        @pl.when(t == 8)
        def _():
            for k in (2, 3):
                local(dp.at[chip_rows(turn(z, k))], dpre_o.at[pl.ds((k - 2) * 2 * B, 2 * B)], 2 + k).start()

            @pl.when((z > 0) & (z < Z - 1))
            def _():
                pv[...] = jnp.zeros(pv.shape, BF16)
                sync(pv, came_o, 1)
            sync(x_ref, dyb.at[pl.ds(0, B)], 1)
            sync(dyb.at[pl.ds(0, B)], xg.at[block_of(spot(1, z, z), c)], 1)

            def flush(m, _):
                ms = cols(m)
                dyb[pl.ds(0, TILE), :] = acc[ms, :].astype(BF16)
                acc[ms, :] = jnp.zeros((TILE, D), F32)
                sync(dyb.at[pl.ds(0, TILE)], dwd_o.at[ms], 1)
                return 0

            lax.fori_loop(0, F // TILE, flush, 0)

        @pl.when(t >= 9)
        def _():
            k = (t - 9) // 2
            odd = (t - 9) % 2
            chip = turn(z, k)
            core = jnp.where(odd == 0, c, 1 - c)

            @pl.when(odd == 1)
            def _():
                for hh in (0, 1):
                    from_partner(1, chip, hh).wait_recv()
            sync(xg.at[block_of(k, core)], dyb.at[pl.ds(0, B)], 1)

            def t4(m, _):
                for i in (0, 1):
                    acc[cols(m), pl.ds(i * F, F)] += lax.dot_general(
                        dyb[pl.ds(0, B), cols(2 * m + i)], dp[block_of(chip, core), :], TN,
                        preferred_element_type=F32)
                return 0

            lax.fori_loop(0, D // (2 * TILE), t4, 0)
        return 0

    lax.fori_loop(0, 13, slot, 0)

    local(acc, part_o, 1).start()
    for k in (2, 3):
        local(dp.at[pl.ds(0, 2 * B)], dpre_o.at[pl.ds(0, 2 * B)], 2 + k).wait()
        for h in (0, 1):
            from_partner(1, turn(z, k), h).wait_recv()
    px_send(0, 3).wait_send()
    for chip in range(Z):
        for h in (0, 1):
            for a in (0, 1):
                to_partner(a, chip, h).wait_send()
            kept = ((z == 1) & (chip == 0)) | ((z == Z - 2) & (chip == Z - 1))

            @pl.when((z != chip) & (jnp.logical_not(kept) if h else (z < Z)))
            def _():
                remote(rout.at[chip, half(h)], rin.at[0, chip, half(h)],
                       rs_s.at[chip, h], rs_r.at[0, chip, h], partner).wait_send()
    for d in (0, 1):
        @pl.when(place[d] == Z - 1)
        def _():
            remote(came_o, came_o, rs_s.at[0, 0], rs_r.at[d, z, 0], partner).wait_recv()
        for s in range(Z - 1):
            @pl.when((place[d] < Z - 1) & (s <= place[d]))
            def _():
                for a in (0, 1):
                    for h in (0, 1):
                        line_send(d, a, s, h).wait_send()
    local(acc, part_o, 1).wait()


def line_step(x, dy, pre, w_in, w_down):
    B, D = dy.shape
    H = B // 2
    R, F = pre.shape
    PAD = -(-B // TILE) * TILE
    hbm = pl.BlockSpec(memory_space=pltpu.HBM)
    sds = jax.ShapeDtypeStruct
    dma = pltpu.SemaphoreType.DMA
    return pl.pallas_call(
        line_kernel,
        out_shape=[
            sds((R, D), BF16), sds((R, D), BF16), sds((R // 2, F), BF16), sds((F, D), BF16), sds((F, D), F32),
            sds((H, D), F32), sds((H, D), F32), sds((H, D), BF16), sds((H, D), BF16),
            sds((2, Z, B, D), BF16), sds((Z, B, D), BF16), sds((Z, B, D), BF16),
        ],
        in_specs=[hbm] * 5,
        out_specs=[hbm] * 12,
        scratch_shapes=[
            pltpu.VMEM((D, F), BF16), pltpu.VMEM((F, D), BF16), pltpu.VMEM((F, D), F32),
            pltpu.VMEM((R, F), BF16), pltpu.VMEM((PAD, D), BF16), pltpu.VMEM((B, F), BF16),
            pltpu.VMEM((PAD, F), BF16), pltpu.VMEM((B, D), BF16), pltpu.VMEM((H, D), BF16),
            pltpu.VMEM((2, H, D), BF16), pltpu.VMEM((H, D), BF16), pltpu.VMEM((H, D), F32),
            dma((2, 2, 3, 2)), dma((2, 2, 3, 2)), dma((2, Z, 2)), dma((2, Z, 2)),
            dma((Z,)), dma((Z,)), dma((Z, 2)), dma((2, Z, 2)), dma((8,)),
        ],
        compiler_params=pltpu.CompilerParams(
            collective_id=0, has_side_effects=True, vmem_limit_bytes=62 * 1024 * 1024
        ),
        cost_estimate=pl.CostEstimate(flops=6 * R * D * F, bytes_accessed=12 * R * D, transcendentals=R * F),
    )(x, dy, pre, w_in, w_down)


def finish_kernel(a_ref, b_ref, part_ref, w_ref, base_ref, came_ref, o_ref, wo_ref, dx_ref):
    rows, width = part_ref.shape[0], b_ref.shape[1]
    for i in (0, 1):
        band = pl.ds(i * rows, rows)
        g = lax.dot_general(a_ref[:, band], b_ref[...], TN, preferred_element_type=F32)
        o_ref[band, :] = (part_ref[:, pl.ds(i * width, width)] + g).astype(o_ref.dtype)
    wo_ref[...] = w_ref[...]

    @pl.when(pl.program_id(0) == 0)
    def _():
        dx_ref[...] = (base_ref[...] + came_ref[...].astype(F32)).astype(dx_ref.dtype)


def finish(x, d_pre, part, dw_down, base, came):
    D = x.shape[1]
    R, F = d_pre.shape
    n = D // (2 * TILE)
    H = came.shape[0]
    sds = jax.ShapeDtypeStruct
    first = pl.BlockSpec((H, D), lambda i: (0, 0))
    band = pl.BlockSpec((F // n, D), lambda i: (i, 0))
    return pl.pallas_call(
        finish_kernel,
        grid=(n,),
        out_shape=[sds((D, F), BF16), sds((F, D), BF16), sds((2 * H, D), BF16)],
        in_specs=[pl.BlockSpec((R, D // n), lambda i: (1, i)), pl.BlockSpec((R, F), lambda i: (0, 0)),
                  band, band, first, first],
        out_specs=[pl.BlockSpec((D // n, F), lambda i: (i, 0)), band, first],
        compiler_params=pltpu.CompilerParams(vmem_limit_bytes=56 * 1024 * 1024),
        cost_estimate=pl.CostEstimate(flops=2 * R * D * F, bytes_accessed=2 * (R * D + R * F + 5 * D * F), transcendentals=0),
    )(x, d_pre, part, dw_down, base, came)


def solution(mesh):
    def body(x, dy, pre, w_in, w_down):
        xg, _, d_pre, dw_down, part, base, late_base, last, came, _, _, _ = line_step(x, dy, pre, w_in, w_down)
        hops = [(2 + c, c) for c in (0, 1)] + [(2 * Z - 4 + c, 2 * Z - 2 + c) for c in (0, 1)]
        late = lax.ppermute(last, "tp", hops)
        dw_in, dw_down, dx = finish(xg, d_pre, part, dw_down, base, came)
        dx = lax.dynamic_update_slice(dx, (late_base + late.astype(F32)).astype(BF16), (came.shape[0], 0))
        return dx, dw_in, dw_down

    rows = P(("dp", "tp"), None)
    return jax.shard_map(
        body, mesh=mesh,
        in_specs=(rows, rows, P("dp", "tp"), P(None, "tp"), P("tp", None)),
        out_specs=(rows, P("dp", "tp"), rows),
        check_vma=False,
    )
```

```python
import functools

import jax
import jax.numpy as jnp
from jax import lax
from jax.experimental import pallas as pl
from jax.experimental.pallas import tpu as pltpu
from jax.sharding import PartitionSpec as P

Z = 4
NT = (((1,), (1,)), ((), ()))
TN = (((0,), (0,)), ((), ()))
F32, BF16 = jnp.float32, jnp.bfloat16
K0 = 0.7978845608028654
K1 = 0.044715
TILE = 256
EARLY, MID = 32, 160


def gelu_and_slope(p):
    p2 = p * p
    t = jnp.tanh(K0 * (p + K1 * (p * p2)))
    cdf = 0.5 * (1.0 + t)
    slope = cdf + (0.5 * p) * (1.0 - t * t) * (K0 * (1.0 + (3.0 * K1) * p2))
    return p * cdf, slope


def line_kernel(
    x_ref, dy_ref, pre_ref, wi_ref, wd_ref,
    xg, dyg, dpre_o, dwd_o, part_o, base_o, late_base_o, mid_o, last_o, came_o, rin, pin, rout,
    wi, wd, acc, dp, dyb, preb, hid, pxb, pv, rv, sb, bb,
    ssem, rsem, ps, pr, pxs, pxr, rs_s, rs_r, lsem,
):
    B, D = dy_ref.shape
    H = B // 2
    F = wd_ref.shape[0]
    PAD = dyb.shape[0]
    early, mid = EARLY, MID
    rest = H - early - mid
    tp = lax.axis_index("tp")
    z, c = tp // 2, tp % 2
    partner = z * 2 + (1 - c)
    arrs, gathered = (dy_ref, x_ref), (dyg, xg)
    sign = (1, -1)
    place = (z, Z - 1 - z)
    ahead = tuple(jnp.clip(tp + 2 * s, 0, 2 * Z - 1) for s in sign)

    def remote(src, dst, send, recv, to):
        return pltpu.make_async_remote_copy(
            src_ref=src, dst_ref=dst, send_sem=send, recv_sem=recv,
            device_id={"tp": to}, device_id_type=pl.DeviceIdType.MESH,
        )

    def local(src, dst, i):
        return pltpu.make_async_copy(src, dst, lsem.at[i])

    def sync(src, dst, i):
        cp = local(src, dst, i)
        cp.start()
        cp.wait()

    def turn(zz, k):
        outer = (zz == 0) | (zz == Z - 1)
        o = jnp.where(outer, k, jnp.where(k < 2, 1 - k, k))
        return jnp.where(zz < 2, o, Z - 1 - o)

    def spot(a, zz, chip):
        if a == 0:
            return chip
        p = jnp.where(zz < 2, chip, Z - 1 - chip)
        outer = (zz == 0) | (zz == Z - 1)
        return jnp.where(outer, p, jnp.where(p < 2, 1 - p, p))

    def rows_of(chip, core, h):
        return pl.ds(pl.multiple_of((chip * 2 + core) * B + h * H, 16), H)

    def block_of(chip, core):
        return pl.ds(pl.multiple_of((chip * 2 + core) * B, 32), B)

    def chip_rows(chip):
        return pl.ds(pl.multiple_of(chip * 2 * B, 64), 2 * B)

    def half(h):
        return pl.ds(pl.multiple_of(h * H, 16), H)

    barrier = pltpu.get_barrier_semaphore()
    pl.semaphore_signal(barrier, inc=1, device_id={"tp": partner}, device_id_type=pl.DeviceIdType.MESH)
    for d in (0, 1):
        @pl.when(place[d] < Z - 1)
        def _():
            pl.semaphore_signal(barrier, inc=1, device_id={"tp": ahead[d]}, device_id_type=pl.DeviceIdType.MESH)
    pl.semaphore_wait(barrier, jnp.where((z > 0) & (z < Z - 1), 3, 2))

    def own_send(d, a, h):
        return remote(arrs[a].at[half(h)], gathered[a].at[rows_of(spot(a, z + sign[d], z), c, h)],
                      ssem.at[d, a, 0, h], rsem.at[d, a, 0, h], ahead[d])

    def line_send(d, a, s, h):
        chip = z - sign[d] * s
        return remote(gathered[a].at[rows_of(spot(a, z, chip), c, h)],
                      gathered[a].at[rows_of(spot(a, z + sign[d], chip), c, h)],
                      ssem.at[d, a, s, h], rsem.at[d, a, s, h], ahead[d])

    def line_arrival(d, a, s, h):
        r = rows_of(spot(a, z, z - sign[d] * s), c, h)
        return remote(gathered[a].at[r], gathered[a].at[r],
                      ssem.at[d, a, 0, h], rsem.at[d, a, s - 1, h], ahead[d])

    def own_to_partner(a, h):
        return remote(arrs[a].at[half(h)], gathered[a].at[rows_of(spot(a, z, z), c, h)],
                      ps.at[a, z, h], pr.at[a, z, h], partner)

    def to_partner(a, chip, h):
        r = rows_of(spot(a, z, chip), c, h)
        return remote(gathered[a].at[r], gathered[a].at[r],
                      ps.at[a, chip, h], pr.at[a, chip, h], partner)

    def from_partner(a, chip, h):
        r = rows_of(spot(a, z, chip), 1 - c, h)
        return remote(gathered[a].at[r], gathered[a].at[r],
                      ps.at[a, chip, h], pr.at[a, chip, h], partner)

    for h in (0, 1):
        for d in (0, 1):
            @pl.when(place[d] < Z - 1)
            def _():
                own_send(d, 0, h).start()
    for h in (0, 1):
        own_to_partner(0, h).start()
    local(wd_ref, wd, 6).start()
    local(wi_ref, wi, 7).start()
    for h in (0, 1):
        own_to_partner(1, h).start()

    dyb[pl.ds(B, PAD - B), :] = jnp.zeros((PAD - B, D), BF16)
    hid[pl.ds(B, PAD - B), :] = jnp.zeros((PAD - B, F), BF16)

    def zero(i, _):
        acc[pl.ds(pl.multiple_of(i * 64, 64), 64), :] = jnp.zeros((64, D), F32)
        return 0

    lax.fori_loop(0, F // 64, zero, 0)
    local(wd_ref, wd, 6).wait()
    local(wi_ref, wi, 7).wait()

    def arrive(d, a, s, h):
        line_arrival(d, a, s, h).wait_recv()

        @pl.when(place[d] < Z - 1)
        def _():
            line_send(d, a, s, h).start()
        to_partner(a, z - sign[d] * s, h).start()

    def px_send(chip, k):
        return remote(pxb, pin.at[chip], pxs.at[k], pxr.at[chip], partner)

    def end_send(d, b):
        return remote(rout.at[b, pl.ds(0, early)], came_o.at[pl.ds(0, early)], rs_s.at[b, 0], rs_r.at[d, b, 0], ahead[d])

    def mid_send(d, b):
        return remote(mid_o, came_o.at[pl.ds(early, mid)], rs_s.at[b, 1], rs_r.at[d, b, 1], ahead[d])

    def cols(n, width=TILE):
        return pl.ds(pl.multiple_of(n * width, width), width)

    def slot(t, _):
        s, h = (t + 1) // 2, (t + 1) % 2
        for d in (0, 1):
            q = place[d]

            @pl.when((t >= 1) & (s <= q))
            def _():
                arrive(d, 0, s, h)

            @pl.when((t >= 1) & (s > q) & (s <= 2 * q))
            def _():
                arrive(d, 1, s - q, h)

            @pl.when((t == 2 * q) & (q < Z - 1))
            def _():
                for hh in (0, 1):
                    own_send(d, 1, hh).start()

        @pl.when(t == 12)
        def _():
            local(acc, part_o, 6).start()

        def rs(j, _):
            outer = (z == 0) | (z == Z - 1)
            u0, u1 = jnp.maximum(t - 4, 0), jnp.maximum(t - 7, 0)
            k = jnp.where(outer, (u0 // 2 + 1) % 4, jnp.where(j == 0, (u1 // 2 + 2) % 4, 1))
            b = jnp.where(z < 2, k, Z - 1 - k)
            hh = jnp.where(outer, u0 % 2, jnp.where(j == 0, u1 % 2, (t + 1) % 2))
            first = jnp.where(outer, 4, jnp.where(j == 0, 7, 9))
            end = jnp.where(outer, jnp.where(j == 0, 12, 0), jnp.where(j == 0, 13, 11))

            @pl.when((t >= first) & (t < end))
            def _():
                inner = (z > 0) & (z < Z - 1)
                has = (inner & (b >= z), inner & (b <= z))

                @pl.when(hh == 0)
                def _():
                    remote(pxb, pin.at[b], pxs.at[0], pxr.at[b], partner).wait_recv()
                local(pin.at[b, half(hh)], pv, 0).start()
                for d in (0, 1):
                    @pl.when(has[d])
                    def _():
                        remote(rin.at[d, b, half(hh)], rin.at[d, b, half(hh)],
                               rs_s.at[b, hh], rs_r.at[d, b, hh], partner).wait_recv()
                        local(rin.at[d, b, half(hh)], rv.at[d], 1 + d).start()

                    @pl.when(jnp.logical_not(has[d]))
                    def _():
                        rv[d] = jnp.zeros(rv.shape[1:], BF16)
                local(pin.at[b, half(hh)], pv, 0).wait()
                for d in (0, 1):
                    @pl.when(has[d])
                    def _():
                        local(rin.at[d, b, half(hh)], rv.at[d], 1 + d).wait()

                def tile(n, _):
                    cs = cols(n)
                    g = lax.dot_general(dp[rows_of(b, c, hh), :], wi[cs, :], NT, preferred_element_type=F32)
                    g = g + pv[:, cs].astype(F32)
                    g = g + (rv[0, :, cs].astype(F32) + rv[1, :, cs].astype(F32))
                    bb[:, cs] = g
                    sb[:, cs] = g.astype(BF16)
                    return 0

                lax.fori_loop(0, D // TILE, tile, 0)
                to_end = ((z == 1) & (b == 0)) | ((z == Z - 2) & (b == Z - 1))
                @pl.when(b == z)
                def _():
                    @pl.when(hh == 0)
                    def _():
                        sync(bb.at[pl.ds(0, early + mid)], base_o, 3)
                        sync(bb.at[pl.ds(early + mid, rest)], late_base_o.at[pl.ds(0, rest)], 3)

                    @pl.when(hh == 1)
                    def _():
                        sync(bb, late_base_o.at[pl.ds(rest, H)], 3)

                @pl.when(to_end)
                def _():
                    @pl.when(hh == 0)
                    def _():
                        sync(sb.at[pl.ds(0, early)], rout.at[b, pl.ds(0, early)], 3)
                        sync(sb.at[pl.ds(early, mid)], mid_o, 3)
                        for d in (0, 1):
                            @pl.when((b > z) if d == 0 else (b < z))
                            def _():
                                end_send(d, b).start()

                                @pl.when(c == 1)
                                def _():
                                    mid_send(d, b).start()
                        sync(sb.at[pl.ds(early + mid, rest)], last_o.at[pl.ds(0, rest)], 3)

                    @pl.when(hh == 1)
                    def _():
                        sync(sb, last_o.at[pl.ds(rest, H)], 3)

                @pl.when((b != z) & jnp.logical_not(to_end))
                def _():
                    sync(sb, rout.at[b, half(hh)], 3)
                    for d in (0, 1):
                        @pl.when((b > z) if d == 0 else (b < z))
                        def _():
                            r_send(d, b, hh).start()
            return 0

        def r_send(d, b, hh):
            return remote(rout.at[b, half(hh)], rin.at[d, b, half(hh)],
                          rs_s.at[b, hh], rs_r.at[d, b, hh], ahead[d])

        lax.fori_loop(0, 2, rs, 0)

        @pl.when(t < 8)
        def _():
            k = t // 2
            chip = turn(z, k)
            odd = t % 2
            core = jnp.where(odd == 0, c, 1 - c)
            blk = block_of(chip, core)
            local(pre_ref.at[blk], preb, 0).start()

            @pl.when(odd == 1)
            def _():
                for hh in (0, 1):
                    from_partner(0, chip, hh).wait_recv()

            @pl.when(t == 0)
            def _():
                sync(dy_ref, dyb.at[pl.ds(0, B)], 1)

            @pl.when(t > 0)
            def _():
                sync(dyg.at[blk], dyb.at[pl.ds(0, B)], 1)
            local(pre_ref.at[blk], preb, 0).wait()

            def t1(n, _):
                cs = cols(n)
                g = lax.dot_general(dyb[pl.ds(0, B), :], wd[cs, :], NT, preferred_element_type=F32)
                hidden, slope = gelu_and_slope(preb[:, cs].astype(F32))
                hid[pl.ds(0, B), cs] = hidden.astype(BF16)
                dp[blk, cs] = (g * slope).astype(BF16)
                return 0

            lax.fori_loop(0, F // TILE, t1, 0)

            @pl.when(odd == 1)
            def _():
                @pl.when(k > 0)
                def _():
                    px_send(chip, k - 1).wait_send()

                def px(n, _):
                    cs = cols(n)
                    g = lax.dot_general(dp[blk, :], wi[cs, :], NT, preferred_element_type=F32)
                    pxb[:, cs] = g.astype(BF16)
                    return 0

                lax.fori_loop(0, D // TILE, px, 0)
                px_send(chip, k).start()

            def t2(m, _):
                ms = cols(m)
                acc[ms, :] += lax.dot_general(hid[:, ms], dyb[...], TN, preferred_element_type=F32)
                return 0

            lax.fori_loop(0, F // TILE, t2, 0)

        @pl.when(t == 8)
        def _():
            for k in (2, 3):
                local(dp.at[chip_rows(turn(z, k))], dpre_o.at[pl.ds((k - 2) * 2 * B, 2 * B)], 2 + k).start()

            pv[...] = jnp.zeros(pv.shape, BF16)

            @pl.when(((z > 0) & (z < Z - 1)) | (c == 0))
            def _():
                sync(pv.at[pl.ds(0, mid)], came_o.at[pl.ds(early, mid)], 1)

            @pl.when((z > 0) & (z < Z - 1))
            def _():
                sync(pv.at[pl.ds(0, early)], came_o.at[pl.ds(0, early)], 1)
            sync(x_ref, dyb.at[pl.ds(0, B)], 1)
            sync(dyb.at[pl.ds(0, B)], xg.at[block_of(spot(1, z, z), c)], 1)

            def flush(m, _):
                ms = cols(m)
                dyb[pl.ds(0, TILE), :] = acc[ms, :].astype(BF16)
                acc[ms, :] = jnp.zeros((TILE, D), F32)
                sync(dyb.at[pl.ds(0, TILE)], dwd_o.at[ms], 1)
                return 0

            lax.fori_loop(0, F // TILE, flush, 0)

        @pl.when((t >= 8) & (t < 12))
        def _():
            k = (t - 8) // 2
            odd = t % 2
            chip = turn(z, k)
            core = jnp.where(odd == 0, c, 1 - c)

            @pl.when(odd == 1)
            def _():
                for hh in (0, 1):
                    from_partner(1, chip, hh).wait_recv()
            sync(xg.at[block_of(k, core)], dyb.at[pl.ds(0, B)], 1)

            def t4(m, _):
                for i in (0, 1):
                    acc[cols(m), pl.ds(i * F, F)] += lax.dot_general(
                        dyb[pl.ds(0, B), cols(2 * m + i)], dp[block_of(chip, core), :], TN,
                        preferred_element_type=F32)
                return 0

            lax.fori_loop(0, D // (2 * TILE), t4, 0)
        return 0

    lax.fori_loop(0, 13, slot, 0)

    for k in (2, 3):
        local(dp.at[pl.ds(0, 2 * B)], dpre_o.at[pl.ds(0, 2 * B)], 2 + k).wait()
        for h in (0, 1):
            from_partner(1, turn(z, k), h).wait_recv()
    px_send(0, 3).wait_send()
    for chip in range(Z):
        for h in (0, 1):
            for a in (0, 1):
                to_partner(a, chip, h).wait_send()
            kept = ((z == 1) & (chip == 0)) | ((z == Z - 2) & (chip == Z - 1))

            @pl.when(kept & ((h == 0) | (c == 1)))
            def _():
                (mid_send if h else end_send)(0, chip).wait_send()

            @pl.when((z != chip) & jnp.logical_not(kept))
            def _():
                remote(rout.at[chip, half(h)], rin.at[0, chip, half(h)],
                       rs_s.at[chip, h], rs_r.at[0, chip, h], partner).wait_send()
    for d in (0, 1):
        @pl.when(place[d] == Z - 1)
        def _():
            end_send(d, z).wait_recv()

            @pl.when(c == 1)
            def _():
                mid_send(d, z).wait_recv()

        for s in range(Z - 1):
            @pl.when((place[d] < Z - 1) & (s <= place[d]))
            def _():
                for a in (0, 1):
                    for h in (0, 1):
                        line_send(d, a, s, h).wait_send()
    local(acc, part_o, 6).wait()


def line_step(x, dy, pre, w_in, w_down):
    B, D = dy.shape
    H = B // 2
    R, F = pre.shape
    PAD = -(-B // TILE) * TILE
    hbm = pl.BlockSpec(memory_space=pltpu.HBM)
    sds = jax.ShapeDtypeStruct
    dma = pltpu.SemaphoreType.DMA
    return pl.pallas_call(
        line_kernel,
        out_shape=[
            sds((R, D), BF16), sds((R, D), BF16), sds((R // 2, F), BF16), sds((F, D), BF16), sds((F, D), F32),
            sds((EARLY + MID, D), F32), sds((B - EARLY - MID, D), F32),
            sds((MID, D), BF16), sds((B - EARLY - MID, D), BF16), sds((EARLY + MID, D), BF16),
            sds((2, Z, B, D), BF16), sds((Z, B, D), BF16), sds((Z, B, D), BF16),
        ],
        in_specs=[hbm] * 5,
        out_specs=[hbm] * 13,
        scratch_shapes=[
            pltpu.VMEM((D, F), BF16), pltpu.VMEM((F, D), BF16), pltpu.VMEM((F, D), F32),
            pltpu.VMEM((R, F), BF16), pltpu.VMEM((PAD, D), BF16), pltpu.VMEM((B, F), BF16),
            pltpu.VMEM((PAD, F), BF16), pltpu.VMEM((B, D), BF16), pltpu.VMEM((H, D), BF16),
            pltpu.VMEM((2, H, D), BF16), pltpu.VMEM((H, D), BF16), pltpu.VMEM((H, D), F32),
            dma((2, 2, 3, 2)), dma((2, 2, 3, 2)), dma((2, Z, 2)), dma((2, Z, 2)),
            dma((Z,)), dma((Z,)), dma((Z, 2)), dma((2, Z, 2)), dma((8,)),
        ],
        compiler_params=pltpu.CompilerParams(
            collective_id=0, has_side_effects=True, vmem_limit_bytes=62 * 1024 * 1024
        ),
        cost_estimate=pl.CostEstimate(flops=6 * R * D * F, bytes_accessed=12 * R * D, transcendentals=R * F),
    )(x, dy, pre, w_in, w_down)


def dw_kernel(a_ref, b_ref, part_ref, o_ref):
    rows, width = part_ref.shape[0], b_ref.shape[1]
    for i in (0, 1):
        band = pl.ds(i * rows, rows)
        g = lax.dot_general(a_ref[:, band], b_ref[...], TN, preferred_element_type=F32)
        o_ref[band, :] = (part_ref[:, pl.ds(i * width, width)] + g).astype(o_ref.dtype)


def finish_dw(x, d_pre, part):
    D = x.shape[1]
    R, F = d_pre.shape
    n = D // (2 * TILE)
    last = x.shape[0] // R - 1
    return pl.pallas_call(
        dw_kernel,
        grid=(n,),
        out_shape=jax.ShapeDtypeStruct((D, F), BF16),
        in_specs=[pl.BlockSpec((R, D // n), lambda i: (last, i)), pl.BlockSpec((R, F), lambda i: (0, 0)),
                  pl.BlockSpec((F // n, D), lambda i: (i, 0))],
        out_specs=pl.BlockSpec((D // n, F), lambda i: (i, 0)),
        compiler_params=pltpu.CompilerParams(vmem_limit_bytes=48 * 1024 * 1024),
        cost_estimate=pl.CostEstimate(flops=2 * R * D * F, bytes_accessed=2 * (R * D + R * F + 3 * D * F), transcendentals=0),
    )(x, d_pre, part)


def pass_kernel(w_ref, base_ref, came_ref, mid_ref, wo_ref, dx_ref):
    wo_ref[...] = w_ref[...]

    @pl.when(pl.program_id(0) == 0)
    def _():
        for first, count, more in ((0, EARLY, None), (EARLY, MID, mid_ref)):
            rows = pl.ds(first, count)
            total = base_ref[rows, :] + came_ref[rows, :].astype(F32)
            if more is not None:
                total = total + more[...].astype(F32)
            dx_ref[rows, :] = total.astype(dx_ref.dtype)


def pass_on(dw_down, base, came, mid, rows):
    F, D = dw_down.shape
    sds = jax.ShapeDtypeStruct
    down = pl.BlockSpec((F // 2, D), lambda i: (i, 0))
    strip = pl.BlockSpec((EARLY + MID, D), lambda i: (0, 0))
    return pl.pallas_call(
        pass_kernel,
        grid=(2,),
        out_shape=[sds((F, D), BF16), sds((rows, D), BF16)],
        in_specs=[down, strip, strip, pl.BlockSpec((MID, D), lambda i: (0, 0))],
        out_specs=[down, strip],
        compiler_params=pltpu.CompilerParams(vmem_limit_bytes=32 * 1024 * 1024),
        cost_estimate=pl.CostEstimate(flops=4 * F * D * 512, bytes_accessed=4 * F * D, transcendentals=0),
    )(dw_down, base, came, mid)


def solution(mesh):
    def body(x, dy, pre, w_in, w_down):
        xg, _, d_pre, dw_down, part, base, late_base, mid, last, came, _, _, _ = line_step(x, dy, pre, w_in, w_down)
        hops = [[(2 + c, c), (2 * Z - 4 + c, 2 * Z - 2 + c)] for c in (0, 1)]
        mid = lax.ppermute(mid, "tp", hops[0])
        last = lax.ppermute(last, "tp", hops[0] + hops[1])
        dw_in = finish_dw(xg, d_pre, part)
        dw_down, dx = pass_on(dw_down, base, came, mid, x.shape[0])
        dx = lax.dynamic_update_slice(dx, (late_base + last.astype(F32)).astype(BF16), (EARLY + MID, 0))
        return dx, dw_in, dw_down

    rows = P(("dp", "tp"), None)
    return jax.shard_map(
        body, mesh=mesh,
        in_specs=(rows, rows, P("dp", "tp"), P(None, "tp"), P("tp", None)),
        out_specs=(rows, P("dp", "tp"), rows),
        check_vma=False,
    )
```

```python
import functools

import jax
import jax.numpy as jnp
from jax import lax
from jax.experimental import pallas as pl
from jax.experimental.pallas import tpu as pltpu
from jax.sharding import PartitionSpec as P

Z = 4
NT = (((1,), (1,)), ((), ()))
TN = (((0,), (0,)), ((), ()))
F32, BF16 = jnp.float32, jnp.bfloat16
K0 = 0.7978845608028654
K1 = 0.044715
TILE = 256
EARLY, MID = 64, 128


def gelu_and_slope(p):
    p2 = p * p
    t = jnp.tanh(K0 * (p + K1 * (p * p2)))
    cdf = 0.5 * (1.0 + t)
    slope = cdf + (0.5 * p) * (1.0 - t * t) * (K0 * (1.0 + (3.0 * K1) * p2))
    return p * cdf, slope


def line_kernel(
    x_ref, dy_ref, pre_ref, wi_ref, wd_ref,
    xg, dyg, dpre_o, dwd_o, part_o, base_o, last_base_o, mid_o, last_o, came_o, rin, pin, rout,
    wi, wd, acc, dp, dyb, preb, hid, pxb, pv, rv, sb, bb,
    ssem, rsem, ps, pr, pxs, pxr, rs_s, rs_r, lsem, in_sem,
):
    B, D = dy_ref.shape
    H = B // 2
    F = wd_ref.shape[0]
    PAD = dyb.shape[0]
    early, mid = EARLY, MID
    rest = H - early - mid
    tp = lax.axis_index("tp")
    z, c = tp // 2, tp % 2
    partner = z * 2 + (1 - c)
    arrs, gathered = (dy_ref, x_ref), (dyg, xg)
    sign = (1, -1)
    place = (z, Z - 1 - z)
    ahead = tuple(jnp.clip(tp + 2 * s, 0, 2 * Z - 1) for s in sign)

    def remote(src, dst, send, recv, to):
        return pltpu.make_async_remote_copy(
            src_ref=src, dst_ref=dst, send_sem=send, recv_sem=recv,
            device_id={"tp": to}, device_id_type=pl.DeviceIdType.MESH,
        )

    def local(src, dst, i):
        return pltpu.make_async_copy(src, dst, lsem.at[i])

    def sync(src, dst, i):
        cp = local(src, dst, i)
        cp.start()
        cp.wait()

    def turn(zz, k):
        outer = (zz == 0) | (zz == Z - 1)
        o = jnp.where(outer, k, jnp.where(k < 2, 1 - k, k))
        return jnp.where(zz < 2, o, Z - 1 - o)

    def spot(a, zz, chip):
        if a == 0:
            return chip
        p = jnp.where(zz < 2, chip, Z - 1 - chip)
        outer = (zz == 0) | (zz == Z - 1)
        return jnp.where(outer, p, jnp.where(p < 2, 1 - p, p))

    def settle():
        sync(pre_ref.at[pl.ds(0, 16)], preb.at[pl.ds(0, 16)], 5)

    def rows_of(chip, core, h):
        return pl.ds(pl.multiple_of((chip * 2 + core) * B + h * H, 16), H)

    def block_of(chip, core):
        return pl.ds(pl.multiple_of((chip * 2 + core) * B, 32), B)

    def chip_rows(chip):
        return pl.ds(pl.multiple_of(chip * 2 * B, 64), 2 * B)

    def half(h):
        return pl.ds(pl.multiple_of(h * H, 16), H)

    def signal(sem, to):
        pl.semaphore_signal(sem, inc=1, device_id={"tp": to}, device_id_type=pl.DeviceIdType.MESH)

    barrier = pltpu.get_barrier_semaphore()
    signal(barrier, partner)
    for d in (0, 1):
        @pl.when((place[d] < Z - 1) & ((d == 0) | (z != 2)))
        def _():
            signal(barrier, ahead[d])
    pl.semaphore_wait(barrier, jnp.where(z == 2, 3, 2))

    @pl.when(z == 2)
    def _():
        signal(in_sem, ahead[1])

    def own_send(d, a, h):
        return remote(arrs[a].at[half(h)], gathered[a].at[rows_of(spot(a, z + sign[d], z), c, h)],
                      ssem.at[d, a, 0, h], rsem.at[d, a, 0, h], ahead[d])

    def line_send(d, a, s, h):
        chip = z - sign[d] * s
        return remote(gathered[a].at[rows_of(spot(a, z, chip), c, h)],
                      gathered[a].at[rows_of(spot(a, z + sign[d], chip), c, h)],
                      ssem.at[d, a, s, h], rsem.at[d, a, s, h], ahead[d])

    def line_arrival(d, a, s, h):
        r = rows_of(spot(a, z, z - sign[d] * s), c, h)
        return remote(gathered[a].at[r], gathered[a].at[r],
                      ssem.at[d, a, 0, h], rsem.at[d, a, s - 1, h], ahead[d])

    def own_to_partner(a, h):
        return remote(arrs[a].at[half(h)], gathered[a].at[rows_of(spot(a, z, z), c, h)],
                      ps.at[a, z, h], pr.at[a, z, h], partner)

    def to_partner(a, chip, h):
        r = rows_of(spot(a, z, chip), c, h)
        return remote(gathered[a].at[r], gathered[a].at[r],
                      ps.at[a, chip, h], pr.at[a, chip, h], partner)

    def from_partner(a, chip, h):
        r = rows_of(spot(a, z, chip), 1 - c, h)
        return remote(gathered[a].at[r], gathered[a].at[r],
                      ps.at[a, chip, h], pr.at[a, chip, h], partner)

    for d in (1, 0):
        @pl.when(place[d] < Z - 1)
        def _():
            if d == 0:
                @pl.when(z == 1)
                def _():
                    pl.semaphore_wait(in_sem, 1)
            for h in (0, 1):
                own_send(d, 0, h).start()
    for h in (0, 1):
        own_to_partner(0, h).start()
    local(wd_ref, wd, 6).start()
    local(wi_ref, wi, 7).start()
    for h in (0, 1):
        own_to_partner(1, h).start()

    dyb[pl.ds(B, PAD - B), :] = jnp.zeros((PAD - B, D), BF16)
    hid[pl.ds(B, PAD - B), :] = jnp.zeros((PAD - B, F), BF16)

    def zero(i, _):
        acc[pl.ds(pl.multiple_of(i * 64, 64), 64), :] = jnp.zeros((64, D), F32)
        return 0

    lax.fori_loop(0, F // 64, zero, 0)
    local(wd_ref, wd, 6).wait()
    local(wi_ref, wi, 7).wait()

    def arrive(d, a, s, h):
        line_arrival(d, a, s, h).wait_recv()

        @pl.when(place[d] < Z - 1)
        def _():
            line_send(d, a, s, h).start()
        to_partner(a, z - sign[d] * s, h).start()

    def px_send(chip, k):
        return remote(pxb, pin.at[chip], pxs.at[k], pxr.at[chip], partner)

    def end_send(d, b):
        return remote(rout.at[b, pl.ds(0, early)], came_o.at[pl.ds(0, early)], rs_s.at[b, 0], rs_r.at[d, b, 0], ahead[d])

    def mid_send(d, b):
        return remote(mid_o, came_o.at[pl.ds(early, mid)], rs_s.at[b, 1], rs_r.at[d, b, 1], ahead[d])

    def cols(n, width=TILE):
        return pl.ds(pl.multiple_of(n * width, width), width)

    def slot(t, _):
        s, h = (t + 1) // 2, (t + 1) % 2
        for d in (0, 1):
            q = place[d]

            @pl.when((t >= 1) & (s <= q))
            def _():
                arrive(d, 0, s, h)

            @pl.when((t >= 1) & (s > q) & (s <= 2 * q))
            def _():
                arrive(d, 1, s - q, h)

            @pl.when((t == 2 * q) & (q < Z - 1))
            def _():
                for hh in (0, 1):
                    own_send(d, 1, hh).start()

        @pl.when(t == 12)
        def _():
            settle()
            local(acc, part_o, 6).start()

        def rs(j, _):
            outer = (z == 0) | (z == Z - 1)
            u0, u1 = jnp.maximum(t - 4, 0), jnp.maximum(t - 7, 0)
            k = jnp.where(outer, (u0 // 2 + 1) % 4, jnp.where(j == 0, (u1 // 2 + 2) % 4, 1))
            b = jnp.where(z < 2, k, Z - 1 - k)
            hh = jnp.where(outer, u0 % 2, jnp.where(j == 0, u1 % 2, (t + 1) % 2))
            first = jnp.where(outer, 4, jnp.where(j == 0, 7, 9))
            end = jnp.where(outer, jnp.where(j == 0, 12, 0), jnp.where(j == 0, 13, 11))

            @pl.when((t >= first) & (t < end))
            def _():
                inner = (z > 0) & (z < Z - 1)
                has = (inner & (b >= z), inner & (b <= z))

                @pl.when(hh == 0)
                def _():
                    remote(pxb, pin.at[b], pxs.at[0], pxr.at[b], partner).wait_recv()
                sync(pin.at[b, half(hh)], pv, 0)

                def own(n, _):
                    cs = cols(n)
                    g = lax.dot_general(dp[rows_of(b, c, hh), :], wi[cs, :], NT, preferred_element_type=F32)
                    bb[:, cs] = g + pv[:, cs].astype(F32)
                    return 0

                lax.fori_loop(0, D // TILE, own, 0)
                for d in (0, 1):
                    @pl.when(has[d])
                    def _():
                        remote(rin.at[d, b, half(hh)], rin.at[d, b, half(hh)],
                               rs_s.at[b, hh], rs_r.at[d, b, hh], partner).wait_recv()
                        local(rin.at[d, b, half(hh)], rv.at[d], 1 + d).start()

                    @pl.when(jnp.logical_not(has[d]))
                    def _():
                        rv[d] = jnp.zeros(rv.shape[1:], BF16)
                for d in (0, 1):
                    @pl.when(has[d])
                    def _():
                        local(rin.at[d, b, half(hh)], rv.at[d], 1 + d).wait()

                def tile(n, _):
                    cs = cols(n)
                    g = bb[:, cs] + (rv[0, :, cs].astype(F32) + rv[1, :, cs].astype(F32))
                    bb[:, cs] = g
                    sb[:, cs] = g.astype(BF16)
                    return 0

                lax.fori_loop(0, D // TILE, tile, 0)
                to_end = ((z == 1) & (b == 0)) | ((z == Z - 2) & (b == Z - 1))
                @pl.when(b == z)
                def _():
                    @pl.when(hh == 0)
                    def _():
                        sync(bb.at[pl.ds(0, early + mid)], base_o, 3)
                        sync(bb.at[pl.ds(early + mid, rest)], last_base_o.at[pl.ds(0, rest)], 3)

                    @pl.when(hh == 1)
                    def _():
                        sync(bb, last_base_o.at[pl.ds(rest, H)], 3)

                @pl.when(to_end)
                def _():
                    @pl.when(hh == 0)
                    def _():
                        sync(sb.at[pl.ds(0, early)], rout.at[b, pl.ds(0, early)], 3)
                        sync(sb.at[pl.ds(early, mid)], mid_o, 3)
                        for d in (0, 1):
                            @pl.when((b > z) if d == 0 else (b < z))
                            def _():
                                end_send(d, b).start()

                                @pl.when(c == 1)
                                def _():
                                    mid_send(d, b).start()
                        sync(sb.at[pl.ds(early + mid, rest)], last_o.at[pl.ds(0, rest)], 3)

                    @pl.when(hh == 1)
                    def _():
                        sync(sb, last_o.at[pl.ds(rest, H)], 3)

                @pl.when((b != z) & jnp.logical_not(to_end))
                def _():
                    sync(sb, rout.at[b, half(hh)], 3)
                    for d in (0, 1):
                        @pl.when((b > z) if d == 0 else (b < z))
                        def _():
                            r_send(d, b, hh).start()
            return 0

        def r_send(d, b, hh):
            return remote(rout.at[b, half(hh)], rin.at[d, b, half(hh)],
                          rs_s.at[b, hh], rs_r.at[d, b, hh], ahead[d])

        lax.fori_loop(0, 2, rs, 0)

        @pl.when(t < 8)
        def _():
            k = t // 2
            chip = turn(z, k)
            odd = t % 2
            core = jnp.where(odd == 0, c, 1 - c)
            blk = block_of(chip, core)
            local(pre_ref.at[blk], preb, 0).start()

            @pl.when(odd == 1)
            def _():
                for hh in (0, 1):
                    from_partner(0, chip, hh).wait_recv()

            @pl.when(t == 0)
            def _():
                sync(dy_ref, dyb.at[pl.ds(0, B)], 1)

            @pl.when(t > 0)
            def _():
                sync(dyg.at[blk], dyb.at[pl.ds(0, B)], 1)
            local(pre_ref.at[blk], preb, 0).wait()

            def t1(n, _):
                cs = cols(n)
                g = lax.dot_general(dyb[pl.ds(0, B), :], wd[cs, :], NT, preferred_element_type=F32)
                hidden, slope = gelu_and_slope(preb[:, cs].astype(F32))
                hid[pl.ds(0, B), cs] = hidden.astype(BF16)
                dp[blk, cs] = (g * slope).astype(BF16)
                return 0

            lax.fori_loop(0, F // TILE, t1, 0)

            @pl.when(odd == 1)
            def _():
                @pl.when(k > 0)
                def _():
                    px_send(chip, k - 1).wait_send()

                def px(n, _):
                    cs = cols(n)
                    g = lax.dot_general(dp[blk, :], wi[cs, :], NT, preferred_element_type=F32)
                    pxb[:, cs] = g.astype(BF16)
                    return 0

                lax.fori_loop(0, D // TILE, px, 0)
                settle()
                px_send(chip, k).start()

            def t2(m, _):
                ms = cols(m)
                acc[ms, :] += lax.dot_general(hid[:, ms], dyb[...], TN, preferred_element_type=F32)
                return 0

            lax.fori_loop(0, F // TILE, t2, 0)

        @pl.when(t == 2)
        def _():
            pv[...] = jnp.zeros(pv.shape, BF16)

            @pl.when(((z > 0) & (z < Z - 1)) | (c == 0))
            def _():
                sync(pv.at[pl.ds(0, mid)], came_o.at[pl.ds(early, mid)], 1)

            @pl.when((z > 0) & (z < Z - 1))
            def _():
                sync(pv.at[pl.ds(0, early)], came_o.at[pl.ds(0, early)], 1)
            sync(x_ref, dyb.at[pl.ds(0, B)], 1)
            sync(dyb.at[pl.ds(0, B)], xg.at[block_of(spot(1, z, z), c)], 1)

        @pl.when(t == 8)
        def _():
            for k in (2, 3):
                local(dp.at[chip_rows(turn(z, k))], dpre_o.at[pl.ds((k - 2) * 2 * B, 2 * B)], 2 + k).start()

            def flush(m, _):
                ms = cols(m)
                dyb[pl.ds(0, TILE), :] = acc[ms, :].astype(BF16)
                acc[ms, :] = jnp.zeros((TILE, D), F32)
                sync(dyb.at[pl.ds(0, TILE)], dwd_o.at[ms], 1)
                return 0

            lax.fori_loop(0, F // TILE, flush, 0)

        @pl.when((t >= 8) & (t < 12))
        def _():
            k = (t - 8) // 2
            odd = t % 2
            chip = turn(z, k)
            core = jnp.where(odd == 0, c, 1 - c)

            @pl.when(odd == 1)
            def _():
                for hh in (0, 1):
                    from_partner(1, chip, hh).wait_recv()
            sync(xg.at[block_of(k, core)], dyb.at[pl.ds(0, B)], 1)

            def t4(m, _):
                for i in (0, 1):
                    acc[cols(m), pl.ds(i * F, F)] += lax.dot_general(
                        dyb[pl.ds(0, B), cols(2 * m + i)], dp[block_of(chip, core), :], TN,
                        preferred_element_type=F32)
                return 0

            lax.fori_loop(0, D // (2 * TILE), t4, 0)
        return 0

    lax.fori_loop(0, 13, slot, 0)

    for k in (2, 3):
        local(dp.at[pl.ds(0, 2 * B)], dpre_o.at[pl.ds(0, 2 * B)], 2 + k).wait()
        for h in (0, 1):
            from_partner(1, turn(z, k), h).wait_recv()
    px_send(0, 3).wait_send()
    for chip in range(Z):
        for h in (0, 1):
            for a in (0, 1):
                to_partner(a, chip, h).wait_send()
            kept = ((z == 1) & (chip == 0)) | ((z == Z - 2) & (chip == Z - 1))

            @pl.when(kept & ((h == 0) | (c == 1)))
            def _():
                (mid_send if h else end_send)(0, chip).wait_send()

            @pl.when((z != chip) & jnp.logical_not(kept))
            def _():
                remote(rout.at[chip, half(h)], rin.at[0, chip, half(h)],
                       rs_s.at[chip, h], rs_r.at[0, chip, h], partner).wait_send()
    for d in (0, 1):
        @pl.when(place[d] == Z - 1)
        def _():
            end_send(d, z).wait_recv()

            @pl.when(c == 1)
            def _():
                mid_send(d, z).wait_recv()

        for s in range(Z - 1):
            @pl.when((place[d] < Z - 1) & (s <= place[d]))
            def _():
                for a in (0, 1):
                    for h in (0, 1):
                        line_send(d, a, s, h).wait_send()
    local(acc, part_o, 6).wait()


def line_step(x, dy, pre, w_in, w_down):
    B, D = dy.shape
    H = B // 2
    R, F = pre.shape
    PAD = -(-B // TILE) * TILE
    hbm = pl.BlockSpec(memory_space=pltpu.HBM)
    sds = jax.ShapeDtypeStruct
    dma = pltpu.SemaphoreType.DMA
    return pl.pallas_call(
        line_kernel,
        out_shape=[
            sds((R, D), BF16), sds((R, D), BF16), sds((R // 2, F), BF16), sds((F, D), BF16), sds((F, D), F32),
            sds((EARLY + MID, D), F32), sds((B - EARLY - MID, D), F32),
            sds((MID, D), BF16), sds((B - EARLY - MID, D), BF16), sds((EARLY + MID, D), BF16),
            sds((2, Z, B, D), BF16), sds((Z, B, D), BF16), sds((Z, B, D), BF16),
        ],
        in_specs=[hbm] * 5,
        out_specs=[hbm] * 13,
        scratch_shapes=[
            pltpu.VMEM((D, F), BF16), pltpu.VMEM((F, D), BF16), pltpu.VMEM((F, D), F32),
            pltpu.VMEM((R, F), BF16), pltpu.VMEM((PAD, D), BF16), pltpu.VMEM((B, F), BF16),
            pltpu.VMEM((PAD, F), BF16), pltpu.VMEM((B, D), BF16), pltpu.VMEM((H, D), BF16),
            pltpu.VMEM((2, H, D), BF16), pltpu.VMEM((H, D), BF16), pltpu.VMEM((H, D), F32),
            dma((2, 2, 3, 2)), dma((2, 2, 3, 2)), dma((2, Z, 2)), dma((2, Z, 2)),
            dma((Z,)), dma((Z,)), dma((Z, 2)), dma((2, Z, 2)), dma((8,)), pltpu.SemaphoreType.REGULAR,
        ],
        compiler_params=pltpu.CompilerParams(
            collective_id=0, has_side_effects=True, vmem_limit_bytes=62 * 1024 * 1024
        ),
        cost_estimate=pl.CostEstimate(flops=6 * R * D * F, bytes_accessed=12 * R * D, transcendentals=R * F),
    )(x, dy, pre, w_in, w_down)


def dw_kernel(a_ref, b_ref, part_ref, o_ref):
    rows, width = part_ref.shape[0], b_ref.shape[1]
    for i in (0, 1):
        band = pl.ds(i * rows, rows)
        g = lax.dot_general(a_ref[:, band], b_ref[...], TN, preferred_element_type=F32)
        o_ref[band, :] = (part_ref[:, pl.ds(i * width, width)] + g).astype(o_ref.dtype)


def finish_dw(x, d_pre, part):
    D = x.shape[1]
    R, F = d_pre.shape
    n = D // (2 * TILE)
    last = x.shape[0] // R - 1
    return pl.pallas_call(
        dw_kernel,
        grid=(n,),
        out_shape=jax.ShapeDtypeStruct((D, F), BF16),
        in_specs=[pl.BlockSpec((R, D // n), lambda i: (last, i)), pl.BlockSpec((R, F), lambda i: (0, 0)),
                  pl.BlockSpec((F // n, D), lambda i: (i, 0))],
        out_specs=pl.BlockSpec((D // n, F), lambda i: (i, 0)),
        compiler_params=pltpu.CompilerParams(vmem_limit_bytes=48 * 1024 * 1024),
        cost_estimate=pl.CostEstimate(flops=2 * R * D * F, bytes_accessed=2 * (R * D + R * F + 3 * D * F), transcendentals=0),
    )(x, d_pre, part)


def pass_kernel(w_ref, base_ref, came_ref, mid_ref, wo_ref, dx_ref):
    wo_ref[...] = w_ref[...]

    @pl.when(pl.program_id(0) == 0)
    def _():
        for first, count, more in ((0, EARLY, None), (EARLY, MID, mid_ref)):
            rows = pl.ds(first, count)
            total = base_ref[rows, :] + came_ref[rows, :].astype(F32)
            if more is not None:
                total = total + more[...].astype(F32)
            dx_ref[rows, :] = total.astype(dx_ref.dtype)


def pass_on(dw_down, base, came, mid, rows):
    F, D = dw_down.shape
    sds = jax.ShapeDtypeStruct
    down = pl.BlockSpec((F // 2, D), lambda i: (i, 0))
    strip = pl.BlockSpec((EARLY + MID, D), lambda i: (0, 0))
    return pl.pallas_call(
        pass_kernel,
        grid=(2,),
        out_shape=[sds((F, D), BF16), sds((rows, D), BF16)],
        in_specs=[down, strip, strip, pl.BlockSpec((MID, D), lambda i: (0, 0))],
        out_specs=[down, strip],
        compiler_params=pltpu.CompilerParams(vmem_limit_bytes=32 * 1024 * 1024),
        cost_estimate=pl.CostEstimate(flops=4 * F * D * 512, bytes_accessed=4 * F * D, transcendentals=0),
    )(dw_down, base, came, mid)


def solution(mesh):
    def body(x, dy, pre, w_in, w_down):
        xg, _, d_pre, dw_down, part, base, last_base, mid, last, came, _, _, _ = line_step(x, dy, pre, w_in, w_down)
        hops = [[(2 + c, c), (2 * Z - 4 + c, 2 * Z - 2 + c)] for c in (0, 1)]
        mid = lax.ppermute(mid, "tp", hops[0])
        last = lax.ppermute(last, "tp", hops[0] + hops[1])
        dw_in = finish_dw(xg, d_pre, part)
        dw_down, dx = pass_on(dw_down, base, came, mid, x.shape[0])
        dx = lax.dynamic_update_slice(dx, (last_base + last.astype(F32)).astype(BF16), (EARLY + MID, 0))
        return dx, dw_in, dw_down

    rows = P(("dp", "tp"), None)
    return jax.shard_map(
        body, mesh=mesh,
        in_specs=(rows, rows, P("dp", "tp"), P(None, "tp"), P("tp", None)),
        out_specs=(rows, P("dp", "tp"), rows),
        check_vma=False,
    )
```

```python
import functools

import jax
import jax.numpy as jnp
from jax import lax
from jax.experimental import pallas as pl
from jax.experimental.pallas import tpu as pltpu
from jax.sharding import PartitionSpec as P

Z = 4
NT = (((1,), (1,)), ((), ()))
TN = (((0,), (0,)), ((), ()))
F32, BF16 = jnp.float32, jnp.bfloat16
K0 = 0.7978845608028654
K1 = 0.044715
TILE = 256
EARLY, MID = 64, 128


def gelu_and_slope(p):
    p2 = p * p
    t = jnp.tanh(K0 * (p + K1 * (p * p2)))
    cdf = 0.5 * (1.0 + t)
    slope = cdf + (0.5 * p) * (1.0 - t * t) * (K0 * (1.0 + (3.0 * K1) * p2))
    return p * cdf, slope


def line_kernel(
    x_ref, dy_ref, pre_ref, wi_ref, wd_ref,
    xg, dyg, dpre_o, dwd_o, part_o, base_o, last_base_o, mid_o, last_o, came_o, rin, pin, rout,
    wi, wd, acc, dp, dyb, preb, hid, pxb, pv, rv, sb, bb,
    ssem, rsem, ps, pr, pxs, pxr, rs_s, rs_r, lsem, in_sem,
):
    B, D = dy_ref.shape
    H = B // 2
    F = wd_ref.shape[0]
    PAD = dyb.shape[0]
    early, mid = EARLY, MID
    rest = H - early - mid
    tp = lax.axis_index("tp")
    z, c = tp // 2, tp % 2
    partner = z * 2 + (1 - c)
    arrs, gathered = (dy_ref, x_ref), (dyg, xg)
    sign = (1, -1)
    place = (z, Z - 1 - z)
    ahead = tuple(jnp.clip(tp + 2 * s, 0, 2 * Z - 1) for s in sign)

    def remote(src, dst, send, recv, to):
        return pltpu.make_async_remote_copy(
            src_ref=src, dst_ref=dst, send_sem=send, recv_sem=recv,
            device_id={"tp": to}, device_id_type=pl.DeviceIdType.MESH,
        )

    def local(src, dst, i):
        return pltpu.make_async_copy(src, dst, lsem.at[i])

    def sync(src, dst, i):
        cp = local(src, dst, i)
        cp.start()
        cp.wait()

    def turn(zz, k):
        outer = (zz == 0) | (zz == Z - 1)
        o = jnp.where(outer, k, jnp.where(k < 2, 1 - k, k))
        return jnp.where(zz < 2, o, Z - 1 - o)

    def spot(a, zz, chip):
        if a == 0:
            return chip
        p = jnp.where(zz < 2, chip, Z - 1 - chip)
        outer = (zz == 0) | (zz == Z - 1)
        return jnp.where(outer, p, jnp.where(p < 2, 1 - p, p))

    def settle():
        sync(hid.at[pl.ds(0, 16), :], rout.at[z, pl.ds(0, 16), pl.ds(0, F)], 8)

    def rows_of(chip, core, h):
        return pl.ds(pl.multiple_of((chip * 2 + core) * B + h * H, 16), H)

    def block_of(chip, core):
        return pl.ds(pl.multiple_of((chip * 2 + core) * B, 32), B)

    def chip_rows(chip):
        return pl.ds(pl.multiple_of(chip * 2 * B, 64), 2 * B)

    def half(h):
        return pl.ds(pl.multiple_of(h * H, 16), H)

    def signal(sem, to):
        pl.semaphore_signal(sem, inc=1, device_id={"tp": to}, device_id_type=pl.DeviceIdType.MESH)

    barrier = pltpu.get_barrier_semaphore()
    signal(barrier, partner)
    for d in (0, 1):
        @pl.when((place[d] < Z - 1) & ((d == 0) | (z != 2)))
        def _():
            signal(barrier, ahead[d])
    pl.semaphore_wait(barrier, jnp.where(z == 2, 3, 2))

    @pl.when(z == 2)
    def _():
        signal(in_sem, ahead[1])

    def own_send(d, a, h):
        return remote(arrs[a].at[half(h)], gathered[a].at[rows_of(spot(a, z + sign[d], z), c, h)],
                      ssem.at[d, a, 0, h], rsem.at[d, a, 0, h], ahead[d])

    def line_send(d, a, s, h):
        chip = z - sign[d] * s
        return remote(gathered[a].at[rows_of(spot(a, z, chip), c, h)],
                      gathered[a].at[rows_of(spot(a, z + sign[d], chip), c, h)],
                      ssem.at[d, a, s, h], rsem.at[d, a, s, h], ahead[d])

    def line_arrival(d, a, s, h):
        r = rows_of(spot(a, z, z - sign[d] * s), c, h)
        return remote(gathered[a].at[r], gathered[a].at[r],
                      ssem.at[d, a, 0, h], rsem.at[d, a, s - 1, h], ahead[d])

    def own_to_partner(a, h):
        return remote(arrs[a].at[half(h)], gathered[a].at[rows_of(spot(a, z, z), c, h)],
                      ps.at[a, z, h], pr.at[a, z, h], partner)

    def to_partner(a, chip, h):
        r = rows_of(spot(a, z, chip), c, h)
        return remote(gathered[a].at[r], gathered[a].at[r],
                      ps.at[a, chip, h], pr.at[a, chip, h], partner)

    def from_partner(a, chip, h):
        r = rows_of(spot(a, z, chip), 1 - c, h)
        return remote(gathered[a].at[r], gathered[a].at[r],
                      ps.at[a, chip, h], pr.at[a, chip, h], partner)

    for d in (1, 0):
        @pl.when(place[d] < Z - 1)
        def _():
            if d == 0:
                @pl.when(z == 1)
                def _():
                    pl.semaphore_wait(in_sem, 1)
            for h in (0, 1):
                own_send(d, 0, h).start()
    for h in (0, 1):
        own_to_partner(0, h).start()
    local(dy_ref, dyb.at[pl.ds(0, B)], 1).start()
    local(pre_ref.at[block_of(z, c)], preb, 0).start()
    local(wd_ref, wd, 10).start()
    local(wi_ref, wi, 11).start()
    local(x_ref, pxb, 12).start()
    for h in (0, 1):
        own_to_partner(1, h).start()

    dyb[pl.ds(B, PAD - B), :] = jnp.zeros((PAD - B, D), BF16)
    hid[pl.ds(B, PAD - B), :] = jnp.zeros((PAD - B, F), BF16)

    def zero(i, _):
        acc[pl.ds(pl.multiple_of(i * 64, 64), 64), :] = jnp.zeros((64, D), F32)
        return 0

    lax.fori_loop(0, F // 64, zero, 0)
    local(wd_ref, wd, 10).wait()
    local(wi_ref, wi, 11).wait()

    def arrive(d, a, s, h):
        line_arrival(d, a, s, h).wait_recv()

        @pl.when(place[d] < Z - 1)
        def _():
            line_send(d, a, s, h).start()
        to_partner(a, z - sign[d] * s, h).start()

    def px_send(chip, k):
        return remote(pxb, pin.at[chip], pxs.at[k], pxr.at[chip], partner)

    def end_send(d, b):
        return remote(rout.at[b, pl.ds(0, early)], came_o.at[pl.ds(0, early)], rs_s.at[b, 0], rs_r.at[d, b, 0], ahead[d])

    def mid_send(d, b):
        return remote(mid_o, came_o.at[pl.ds(early, mid)], rs_s.at[b, 1], rs_r.at[d, b, 1], ahead[d])

    def cols(n, width=TILE):
        return pl.ds(pl.multiple_of(n * width, width), width)

    def slot(t, _):
        s, h = (t + 1) // 2, (t + 1) % 2
        for d in (0, 1):
            q = place[d]

            @pl.when((t >= 1) & (s <= q))
            def _():
                arrive(d, 0, s, h)

            @pl.when((t >= 1) & (s > q) & (s <= 2 * q))
            def _():
                arrive(d, 1, s - q, h)

            @pl.when((t == 2 * q) & (q < Z - 1))
            def _():
                for hh in (0, 1):
                    own_send(d, 1, hh).start()

        @pl.when(t == 12)
        def _():
            settle()
            local(acc, part_o, 9).start()

        def start_load(a, k):
            core = jnp.where(t % 2 == 0, c, 1 - c)
            chip = turn(z, k)

            @pl.when(t % 2 == 1)
            def _():
                for hh in (0, 1):
                    from_partner(a, chip, hh).wait_recv()
            local(gathered[a].at[block_of(spot(a, z, chip), core)], dyb.at[pl.ds(0, B)], 1).start()

        @pl.when((t > 0) & (t < 8))
        def _():
            start_load(0, t // 2)

        @pl.when((t >= 8) & (t < 12))
        def _():
            start_load(1, (t - 8) // 2)

        def rs(j, _):
            outer = (z == 0) | (z == Z - 1)
            u0, u1 = jnp.maximum(t - 4, 0), jnp.maximum(t - 7, 0)
            k = jnp.where(outer, (u0 // 2 + 1) % 4, jnp.where(j == 0, (u1 // 2 + 2) % 4, 1))
            b = jnp.where(z < 2, k, Z - 1 - k)
            hh = jnp.where(outer, u0 % 2, jnp.where(j == 0, u1 % 2, (t + 1) % 2))
            first = jnp.where(outer, 4, jnp.where(j == 0, 7, 9))
            end = jnp.where(outer, jnp.where(j == 0, 12, 0), jnp.where(j == 0, 13, 11))

            @pl.when((t >= first) & (t < end))
            def _():
                inner = (z > 0) & (z < Z - 1)
                has = (inner & (b >= z), inner & (b <= z))

                @pl.when(hh == 0)
                def _():
                    remote(pxb, pin.at[b], pxs.at[0], pxr.at[b], partner).wait_recv()
                local(pin.at[b, half(hh)], pv, 4).start()
                for d in (0, 1):
                    @pl.when(has[d])
                    def _():
                        remote(rin.at[d, b, half(hh)], rin.at[d, b, half(hh)],
                               rs_s.at[b, hh], rs_r.at[d, b, hh], partner).wait_recv()
                        local(rin.at[d, b, half(hh)], rv.at[d], 5 + d).start()

                    @pl.when(jnp.logical_not(has[d]))
                    def _():
                        rv[d] = jnp.zeros(rv.shape[1:], BF16)

                def own(n, _):
                    cs = cols(n)
                    bb[:, cs] = lax.dot_general(
                        dp[rows_of(b, c, hh), :], wi[cs, :], NT, preferred_element_type=F32)
                    return 0

                lax.fori_loop(0, D // TILE, own, 0)
                local(pin.at[b, half(hh)], pv, 4).wait()
                for d in (0, 1):
                    @pl.when(has[d])
                    def _():
                        local(rin.at[d, b, half(hh)], rv.at[d], 5 + d).wait()

                def tile(n, _):
                    cs = cols(n)
                    g = bb[:, cs] + pv[:, cs].astype(F32)
                    g = g + (rv[0, :, cs].astype(F32) + rv[1, :, cs].astype(F32))
                    bb[:, cs] = g
                    sb[:, cs] = g.astype(BF16)
                    return 0

                lax.fori_loop(0, D // TILE, tile, 0)
                to_end = ((z == 1) & (b == 0)) | ((z == Z - 2) & (b == Z - 1))
                @pl.when(b == z)
                def _():
                    @pl.when(hh == 0)
                    def _():
                        sync(bb.at[pl.ds(0, early + mid)], base_o, 7)
                        sync(bb.at[pl.ds(early + mid, rest)], last_base_o.at[pl.ds(0, rest)], 7)

                    @pl.when(hh == 1)
                    def _():
                        sync(bb, last_base_o.at[pl.ds(rest, H)], 7)

                @pl.when(to_end)
                def _():
                    @pl.when(hh == 0)
                    def _():
                        sync(sb.at[pl.ds(0, early)], rout.at[b, pl.ds(0, early)], 7)
                        sync(sb.at[pl.ds(early, mid)], mid_o, 7)
                        for d in (0, 1):
                            @pl.when((b > z) if d == 0 else (b < z))
                            def _():
                                end_send(d, b).start()

                                @pl.when(c == 1)
                                def _():
                                    mid_send(d, b).start()
                        sync(sb.at[pl.ds(early + mid, rest)], last_o.at[pl.ds(0, rest)], 7)

                    @pl.when(hh == 1)
                    def _():
                        sync(sb, last_o.at[pl.ds(rest, H)], 7)

                @pl.when((b != z) & jnp.logical_not(to_end))
                def _():
                    sync(sb, rout.at[b, half(hh)], 7)
                    for d in (0, 1):
                        @pl.when((b > z) if d == 0 else (b < z))
                        def _():
                            r_send(d, b, hh).start()
            return 0

        def r_send(d, b, hh):
            return remote(rout.at[b, half(hh)], rin.at[d, b, half(hh)],
                          rs_s.at[b, hh], rs_r.at[d, b, hh], ahead[d])

        lax.fori_loop(0, 2, rs, 0)

        @pl.when(t < 8)
        def _():
            k = t // 2
            chip = turn(z, k)
            odd = t % 2
            core = jnp.where(odd == 0, c, 1 - c)
            blk = block_of(chip, core)
            local(pre_ref.at[blk], preb, 0).wait()
            local(dy_ref, dyb.at[pl.ds(0, B)], 1).wait()

            def t1(n, _):
                cs = cols(n)
                g = lax.dot_general(dyb[pl.ds(0, B), :], wd[cs, :], NT, preferred_element_type=F32)
                hidden, slope = gelu_and_slope(preb[:, cs].astype(F32))
                hid[pl.ds(0, B), cs] = hidden.astype(BF16)
                dp[blk, cs] = (g * slope).astype(BF16)
                return 0

            lax.fori_loop(0, F // TILE, t1, 0)

            @pl.when(t < 7)
            def _():
                core = jnp.where(odd == 1, c, 1 - c)
                local(pre_ref.at[block_of(turn(z, (t + 1) // 2), core)], preb, 0).start()

            @pl.when(t == 0)
            def _():
                local(x_ref, pxb, 12).wait()
                local(pxb, xg.at[block_of(spot(1, z, z), c)], 12).start()

            @pl.when(odd == 1)
            def _():
                @pl.when(k == 0)
                def _():
                    local(pxb, xg.at[block_of(spot(1, z, z), c)], 12).wait()

                @pl.when(k > 0)
                def _():
                    px_send(chip, k - 1).wait_send()

                def px(n, _):
                    cs = cols(n)
                    g = lax.dot_general(dp[blk, :], wi[cs, :], NT, preferred_element_type=F32)
                    pxb[:, cs] = g.astype(BF16)
                    return 0

                lax.fori_loop(0, D // TILE, px, 0)
                settle()
                px_send(chip, k).start()

            def t2(m, _):
                ms = cols(m)
                acc[ms, :] += lax.dot_general(hid[:, ms], dyb[...], TN, preferred_element_type=F32)
                return 0

            lax.fori_loop(0, F // TILE, t2, 0)

        @pl.when(t == 2)
        def _():
            pv[...] = jnp.zeros(pv.shape, BF16)

            @pl.when(((z > 0) & (z < Z - 1)) | (c == 0))
            def _():
                sync(pv.at[pl.ds(0, mid)], came_o.at[pl.ds(early, mid)], 13)

            @pl.when((z > 0) & (z < Z - 1))
            def _():
                sync(pv.at[pl.ds(0, early)], came_o.at[pl.ds(0, early)], 13)

        @pl.when(t == 8)
        def _():
            for k in (2, 3):
                local(dp.at[chip_rows(turn(z, k))], dpre_o.at[pl.ds((k - 2) * 2 * B, 2 * B)], k).start()
            px_send(0, 3).wait_send()

            def flush(m, _):
                ms = cols(m)
                pxb[pl.ds(0, TILE), :] = acc[ms, :].astype(BF16)
                acc[ms, :] = jnp.zeros((TILE, D), F32)
                sync(pxb.at[pl.ds(0, TILE)], dwd_o.at[ms], 13)
                return 0

            lax.fori_loop(0, F // TILE, flush, 0)

        @pl.when((t >= 8) & (t < 12))
        def _():
            k = (t - 8) // 2
            chip = turn(z, k)
            core = jnp.where(t % 2 == 0, c, 1 - c)
            local(x_ref, dyb.at[pl.ds(0, B)], 1).wait()

            def t4(m, _):
                for i in (0, 1):
                    acc[cols(m), pl.ds(i * F, F)] += lax.dot_general(
                        dyb[pl.ds(0, B), cols(2 * m + i)], dp[block_of(chip, core), :], TN,
                        preferred_element_type=F32)
                return 0

            lax.fori_loop(0, D // (2 * TILE), t4, 0)
        return 0

    lax.fori_loop(0, 13, slot, 0)

    for k in (2, 3):
        local(dp.at[pl.ds(0, 2 * B)], dpre_o.at[pl.ds(0, 2 * B)], k).wait()
        for h in (0, 1):
            from_partner(1, turn(z, k), h).wait_recv()
    for chip in range(Z):
        for h in (0, 1):
            for a in (0, 1):
                to_partner(a, chip, h).wait_send()
            kept = ((z == 1) & (chip == 0)) | ((z == Z - 2) & (chip == Z - 1))

            @pl.when(kept & ((h == 0) | (c == 1)))
            def _():
                (mid_send if h else end_send)(0, chip).wait_send()

            @pl.when((z != chip) & jnp.logical_not(kept))
            def _():
                remote(rout.at[chip, half(h)], rin.at[0, chip, half(h)],
                       rs_s.at[chip, h], rs_r.at[0, chip, h], partner).wait_send()
    for d in (0, 1):
        @pl.when(place[d] == Z - 1)
        def _():
            end_send(d, z).wait_recv()

            @pl.when(c == 1)
            def _():
                mid_send(d, z).wait_recv()

        for s in range(Z - 1):
            @pl.when((place[d] < Z - 1) & (s <= place[d]))
            def _():
                for a in (0, 1):
                    for h in (0, 1):
                        line_send(d, a, s, h).wait_send()
    local(acc, part_o, 9).wait()


def line_step(x, dy, pre, w_in, w_down):
    B, D = dy.shape
    H = B // 2
    R, F = pre.shape
    PAD = -(-B // TILE) * TILE
    hbm = pl.BlockSpec(memory_space=pltpu.HBM)
    sds = jax.ShapeDtypeStruct
    dma = pltpu.SemaphoreType.DMA
    return pl.pallas_call(
        line_kernel,
        out_shape=[
            sds((R, D), BF16), sds((R, D), BF16), sds((R // 2, F), BF16), sds((F, D), BF16), sds((F, D), F32),
            sds((EARLY + MID, D), F32), sds((B - EARLY - MID, D), F32),
            sds((MID, D), BF16), sds((B - EARLY - MID, D), BF16), sds((EARLY + MID, D), BF16),
            sds((2, Z, B, D), BF16), sds((Z, B, D), BF16), sds((Z, B, D), BF16),
        ],
        in_specs=[hbm] * 5,
        out_specs=[hbm] * 13,
        scratch_shapes=[
            pltpu.VMEM((D, F), BF16), pltpu.VMEM((F, D), BF16), pltpu.VMEM((F, D), F32),
            pltpu.VMEM((R, F), BF16), pltpu.VMEM((PAD, D), BF16), pltpu.VMEM((B, F), BF16),
            pltpu.VMEM((PAD, F), BF16), pltpu.VMEM((B, D), BF16), pltpu.VMEM((H, D), BF16),
            pltpu.VMEM((2, H, D), BF16), pltpu.VMEM((H, D), BF16), pltpu.VMEM((H, D), F32),
            dma((2, 2, 3, 2)), dma((2, 2, 3, 2)), dma((2, Z, 2)), dma((2, Z, 2)),
            dma((Z,)), dma((Z,)), dma((Z, 2)), dma((2, Z, 2)), dma((14,)), pltpu.SemaphoreType.REGULAR,
        ],
        compiler_params=pltpu.CompilerParams(
            collective_id=0, has_side_effects=True, vmem_limit_bytes=62 * 1024 * 1024
        ),
        cost_estimate=pl.CostEstimate(flops=6 * R * D * F, bytes_accessed=12 * R * D, transcendentals=R * F),
    )(x, dy, pre, w_in, w_down)


def dw_kernel(a_ref, b_ref, part_ref, o_ref):
    rows, width = part_ref.shape[0], b_ref.shape[1]
    for i in (0, 1):
        band = pl.ds(i * rows, rows)
        g = lax.dot_general(a_ref[:, band], b_ref[...], TN, preferred_element_type=F32)
        o_ref[band, :] = (part_ref[:, pl.ds(i * width, width)] + g).astype(o_ref.dtype)


def finish_dw(x, d_pre, part):
    D = x.shape[1]
    R, F = d_pre.shape
    n = D // (2 * TILE)
    last = x.shape[0] // R - 1
    return pl.pallas_call(
        dw_kernel,
        grid=(n,),
        out_shape=jax.ShapeDtypeStruct((D, F), BF16),
        in_specs=[pl.BlockSpec((R, D // n), lambda i: (last, i)), pl.BlockSpec((R, F), lambda i: (0, 0)),
                  pl.BlockSpec((F // n, D), lambda i: (i, 0))],
        out_specs=pl.BlockSpec((D // n, F), lambda i: (i, 0)),
        compiler_params=pltpu.CompilerParams(vmem_limit_bytes=48 * 1024 * 1024),
        cost_estimate=pl.CostEstimate(flops=2 * R * D * F, bytes_accessed=2 * (R * D + R * F + 3 * D * F), transcendentals=0),
    )(x, d_pre, part)


def pass_kernel(w_ref, base_ref, came_ref, mid_ref, wo_ref, dx_ref):
    wo_ref[...] = w_ref[...]

    @pl.when(pl.program_id(0) == 0)
    def _():
        for first, count, more in ((0, EARLY, None), (EARLY, MID, mid_ref)):
            rows = pl.ds(first, count)
            total = base_ref[rows, :] + came_ref[rows, :].astype(F32)
            if more is not None:
                total = total + more[...].astype(F32)
            dx_ref[rows, :] = total.astype(dx_ref.dtype)


def pass_on(dw_down, base, came, mid, rows):
    F, D = dw_down.shape
    sds = jax.ShapeDtypeStruct
    down = pl.BlockSpec((F // 2, D), lambda i: (i, 0))
    strip = pl.BlockSpec((EARLY + MID, D), lambda i: (0, 0))
    return pl.pallas_call(
        pass_kernel,
        grid=(2,),
        out_shape=[sds((F, D), BF16), sds((rows, D), BF16)],
        in_specs=[down, strip, strip, pl.BlockSpec((MID, D), lambda i: (0, 0))],
        out_specs=[down, strip],
        compiler_params=pltpu.CompilerParams(vmem_limit_bytes=32 * 1024 * 1024),
        cost_estimate=pl.CostEstimate(flops=4 * F * D * 512, bytes_accessed=4 * F * D, transcendentals=0),
    )(dw_down, base, came, mid)


def solution(mesh):
    def body(x, dy, pre, w_in, w_down):
        xg, _, d_pre, dw_down, part, base, last_base, mid, last, came, _, _, _ = line_step(x, dy, pre, w_in, w_down)
        hops = [[(2 + c, c), (2 * Z - 4 + c, 2 * Z - 2 + c)] for c in (0, 1)]
        mid = lax.ppermute(mid, "tp", hops[0])
        last = lax.ppermute(last, "tp", hops[0] + hops[1])
        dw_in = finish_dw(xg, d_pre, part)
        dw_down, dx = pass_on(dw_down, base, came, mid, x.shape[0])
        dx = lax.dynamic_update_slice(dx, (last_base + last.astype(F32)).astype(BF16), (EARLY + MID, 0))
        return dx, dw_in, dw_down

    rows = P(("dp", "tp"), None)
    return jax.shard_map(
        body, mesh=mesh,
        in_specs=(rows, rows, P("dp", "tp"), P(None, "tp"), P("tp", None)),
        out_specs=(rows, P("dp", "tp"), rows),
        check_vma=False,
    )
```

```python
import functools

import jax
import jax.numpy as jnp
from jax import lax
from jax.experimental import pallas as pl
from jax.experimental.pallas import tpu as pltpu
from jax.sharding import PartitionSpec as P

Z = 4
NT = (((1,), (1,)), ((), ()))
TN = (((0,), (0,)), ((), ()))
F32, BF16 = jnp.float32, jnp.bfloat16
K0 = 0.7978845608028654
K1 = 0.044715
TILE = 256
EARLY, MID = 64, 128


def gelu_and_slope(p):
    p2 = p * p
    t = jnp.tanh(K0 * (p + K1 * (p * p2)))
    cdf = 0.5 * (1.0 + t)
    slope = cdf + (0.5 * p) * (1.0 - t * t) * (K0 * (1.0 + (3.0 * K1) * p2))
    return p * cdf, slope


def line_kernel(
    x_ref, dy_ref, pre_ref, wi_ref, wd_ref,
    xg, dyg, dpre_o, dwd_o, part_o, base_o, last_base_o, mid_o, last_o, came_o, rin, pin, rout,
    wi, wd, acc, dp, dyb, preb, hid, pxb, pv, rv, sb, bb,
    ssem, rsem, ps, pr, pxs, pxr, rs_s, rs_r, lsem, in_sem,
):
    B, D = dy_ref.shape
    H = B // 2
    F = wd_ref.shape[0]
    PAD = dyb.shape[0]
    early, mid = EARLY, MID
    rest = H - early - mid
    tp = lax.axis_index("tp")
    z, c = tp // 2, tp % 2
    partner = z * 2 + (1 - c)
    arrs, gathered = (dy_ref, x_ref), (dyg, xg)
    sign = (1, -1)
    place = (z, Z - 1 - z)
    ahead = tuple(jnp.clip(tp + 2 * s, 0, 2 * Z - 1) for s in sign)

    def remote(src, dst, send, recv, to):
        return pltpu.make_async_remote_copy(
            src_ref=src, dst_ref=dst, send_sem=send, recv_sem=recv,
            device_id={"tp": to}, device_id_type=pl.DeviceIdType.MESH,
        )

    def local(src, dst, i):
        return pltpu.make_async_copy(src, dst, lsem.at[i])

    def sync(src, dst, i):
        cp = local(src, dst, i)
        cp.start()
        cp.wait()

    def turn(zz, k):
        outer = (zz == 0) | (zz == Z - 1)
        o = jnp.where(outer, k, jnp.where(k < 2, 1 - k, k))
        return jnp.where(zz < 2, o, Z - 1 - o)

    def spot(a, zz, chip):
        if a == 0:
            return chip
        p = jnp.where(zz < 2, chip, Z - 1 - chip)
        outer = (zz == 0) | (zz == Z - 1)
        return jnp.where(outer, p, jnp.where(p < 2, 1 - p, p))

    def settle():
        sync(hid.at[pl.ds(0, 16), :], rout.at[z, pl.ds(0, 16), pl.ds(0, F)], 8)

    def rows_of(chip, core, h):
        return pl.ds(pl.multiple_of((chip * 2 + core) * B + h * H, 16), H)

    def block_of(chip, core):
        return pl.ds(pl.multiple_of((chip * 2 + core) * B, 32), B)

    def chip_rows(chip):
        return pl.ds(pl.multiple_of(chip * 2 * B, 64), 2 * B)

    def half(h):
        return pl.ds(pl.multiple_of(h * H, 16), H)

    def signal(sem, to):
        pl.semaphore_signal(sem, inc=1, device_id={"tp": to}, device_id_type=pl.DeviceIdType.MESH)

    barrier = pltpu.get_barrier_semaphore()

    @pl.when((z != 1) | (c == 1))
    def _():
        signal(barrier, partner)
    for d in (0, 1):
        @pl.when((place[d] < Z - 1) & ((d == 0) | (z != 2)))
        def _():
            signal(barrier, ahead[d])
    pl.semaphore_wait(barrier, jnp.where(z == 2, 3, jnp.where((z == 1) & (c == 1), 1, 2)))

    @pl.when(z == 2)
    def _():
        signal(in_sem, ahead[1])

    @pl.when((z == 1) & (c == 0))
    def _():
        signal(in_sem, partner)

    def own_send(d, a, h):
        return remote(arrs[a].at[half(h)], gathered[a].at[rows_of(spot(a, z + sign[d], z), c, h)],
                      ssem.at[d, a, 0, h], rsem.at[d, a, 0, h], ahead[d])

    def line_send(d, a, s, h):
        chip = z - sign[d] * s
        return remote(gathered[a].at[rows_of(spot(a, z, chip), c, h)],
                      gathered[a].at[rows_of(spot(a, z + sign[d], chip), c, h)],
                      ssem.at[d, a, s, h], rsem.at[d, a, s, h], ahead[d])

    def line_arrival(d, a, s, h):
        r = rows_of(spot(a, z, z - sign[d] * s), c, h)
        return remote(gathered[a].at[r], gathered[a].at[r],
                      ssem.at[d, a, 0, h], rsem.at[d, a, s - 1, h], ahead[d])

    def own_to_partner(a, h):
        return remote(arrs[a].at[half(h)], gathered[a].at[rows_of(spot(a, z, z), c, h)],
                      ps.at[a, z, h], pr.at[a, z, h], partner)

    def to_partner(a, chip, h):
        r = rows_of(spot(a, z, chip), c, h)
        return remote(gathered[a].at[r], gathered[a].at[r],
                      ps.at[a, chip, h], pr.at[a, chip, h], partner)

    def from_partner(a, chip, h):
        r = rows_of(spot(a, z, chip), 1 - c, h)
        return remote(gathered[a].at[r], gathered[a].at[r],
                      ps.at[a, chip, h], pr.at[a, chip, h], partner)

    for d in (1, 0):
        @pl.when(place[d] < Z - 1)
        def _():
            if d == 0:
                @pl.when(z == 1)
                def _():
                    pl.semaphore_wait(in_sem, 1 + c)
            for h in (0, 1):
                own_send(d, 0, h).start()
    for h in (0, 1):
        own_to_partner(0, h).start()
    local(dy_ref, dyb.at[pl.ds(0, B)], 1).start()
    local(pre_ref.at[block_of(z, c)], preb, 0).start()
    local(wd_ref, wd, 10).start()
    local(wi_ref, wi, 11).start()
    local(x_ref, pxb, 12).start()
    for h in (0, 1):
        own_to_partner(1, h).start()

    dyb[pl.ds(B, PAD - B), :] = jnp.zeros((PAD - B, D), BF16)
    hid[pl.ds(B, PAD - B), :] = jnp.zeros((PAD - B, F), BF16)

    def zero(i, _):
        acc[pl.ds(pl.multiple_of(i * 64, 64), 64), :] = jnp.zeros((64, D), F32)
        return 0

    lax.fori_loop(0, F // 64, zero, 0)
    local(wd_ref, wd, 10).wait()
    local(wi_ref, wi, 11).wait()

    def arrive(d, a, s, h):
        line_arrival(d, a, s, h).wait_recv()

        @pl.when(place[d] < Z - 1)
        def _():
            line_send(d, a, s, h).start()
        to_partner(a, z - sign[d] * s, h).start()

    def px_send(chip, k):
        return remote(pxb, pin.at[chip], pxs.at[k], pxr.at[chip], partner)

    def end_send(d, b):
        return remote(rout.at[b, pl.ds(0, early)], came_o.at[pl.ds(0, early)], rs_s.at[b, 0], rs_r.at[d, b, 0], ahead[d])

    def mid_send(d, b):
        return remote(mid_o, came_o.at[pl.ds(early, mid)], rs_s.at[b, 1], rs_r.at[d, b, 1], ahead[d])

    def cols(n, width=TILE):
        return pl.ds(pl.multiple_of(n * width, width), width)

    def slot(t, _):
        s, h = (t + 1) // 2, (t + 1) % 2
        for d in (0, 1):
            q = place[d]

            @pl.when((t >= 1) & (s <= q))
            def _():
                arrive(d, 0, s, h)

            @pl.when((t >= 1) & (s > q) & (s <= 2 * q))
            def _():
                arrive(d, 1, s - q, h)

            @pl.when((t == 2 * q) & (q < Z - 1))
            def _():
                for hh in (0, 1):
                    own_send(d, 1, hh).start()

        @pl.when(t == 12)
        def _():
            settle()
            local(acc, part_o, 9).start()

        def start_load(a, k):
            core = jnp.where(t % 2 == 0, c, 1 - c)
            chip = turn(z, k)

            @pl.when(t % 2 == 1)
            def _():
                for hh in (0, 1):
                    from_partner(a, chip, hh).wait_recv()
            local(gathered[a].at[block_of(spot(a, z, chip), core)], dyb.at[pl.ds(0, B)], 1).start()

        @pl.when((t > 0) & (t < 8))
        def _():
            start_load(0, t // 2)

        @pl.when((t >= 8) & (t < 12))
        def _():
            start_load(1, (t - 8) // 2)

        def rs(j, _):
            outer = (z == 0) | (z == Z - 1)
            u0, u1 = jnp.maximum(t - 4, 0), jnp.maximum(t - 7, 0)
            k = jnp.where(outer, (u0 // 2 + 1) % 4, jnp.where(j == 0, (u1 // 2 + 2) % 4, 1))
            b = jnp.where(z < 2, k, Z - 1 - k)
            hh = jnp.where(outer, u0 % 2, jnp.where(j == 0, u1 % 2, (t + 1) % 2))
            first = jnp.where(outer, 4, jnp.where(j == 0, 7, 9))
            end = jnp.where(outer, jnp.where(j == 0, 12, 0), jnp.where(j == 0, 13, 11))

            @pl.when((t >= first) & (t < end))
            def _():
                inner = (z > 0) & (z < Z - 1)
                has = (inner & (b >= z), inner & (b <= z))

                @pl.when(hh == 0)
                def _():
                    remote(pxb, pin.at[b], pxs.at[0], pxr.at[b], partner).wait_recv()
                local(pin.at[b, half(hh)], pv, 4).start()
                for d in (0, 1):
                    @pl.when(has[d])
                    def _():
                        remote(rin.at[d, b, half(hh)], rin.at[d, b, half(hh)],
                               rs_s.at[b, hh], rs_r.at[d, b, hh], partner).wait_recv()
                        local(rin.at[d, b, half(hh)], rv.at[d], 5 + d).start()

                    @pl.when(jnp.logical_not(has[d]))
                    def _():
                        rv[d] = jnp.zeros(rv.shape[1:], BF16)

                def own(n, _):
                    cs = cols(n)
                    bb[:, cs] = lax.dot_general(
                        dp[rows_of(b, c, hh), :], wi[cs, :], NT, preferred_element_type=F32)
                    return 0

                lax.fori_loop(0, D // TILE, own, 0)
                local(pin.at[b, half(hh)], pv, 4).wait()
                for d in (0, 1):
                    @pl.when(has[d])
                    def _():
                        local(rin.at[d, b, half(hh)], rv.at[d], 5 + d).wait()

                def tile(n, _):
                    cs = cols(n)
                    g = bb[:, cs] + pv[:, cs].astype(F32)
                    g = g + (rv[0, :, cs].astype(F32) + rv[1, :, cs].astype(F32))
                    bb[:, cs] = g
                    sb[:, cs] = g.astype(BF16)
                    return 0

                lax.fori_loop(0, D // TILE, tile, 0)
                to_end = ((z == 1) & (b == 0)) | ((z == Z - 2) & (b == Z - 1))
                @pl.when(b == z)
                def _():
                    @pl.when(hh == 0)
                    def _():
                        sync(bb.at[pl.ds(0, early + mid)], base_o, 7)
                        sync(bb.at[pl.ds(early + mid, rest)], last_base_o.at[pl.ds(0, rest)], 7)

                    @pl.when(hh == 1)
                    def _():
                        sync(bb, last_base_o.at[pl.ds(rest, H)], 7)

                @pl.when(to_end)
                def _():
                    @pl.when(hh == 0)
                    def _():
                        sync(sb.at[pl.ds(0, early)], rout.at[b, pl.ds(0, early)], 7)
                        sync(sb.at[pl.ds(early, mid)], mid_o, 7)
                        for d in (0, 1):
                            @pl.when((b > z) if d == 0 else (b < z))
                            def _():
                                end_send(d, b).start()

                                @pl.when(c == 1)
                                def _():
                                    mid_send(d, b).start()
                        sync(sb.at[pl.ds(early + mid, rest)], last_o.at[pl.ds(0, rest)], 7)

                    @pl.when(hh == 1)
                    def _():
                        sync(sb, last_o.at[pl.ds(rest, H)], 7)

                @pl.when((b != z) & jnp.logical_not(to_end))
                def _():
                    sync(sb, rout.at[b, half(hh)], 7)
                    for d in (0, 1):
                        @pl.when((b > z) if d == 0 else (b < z))
                        def _():
                            r_send(d, b, hh).start()
            return 0

        def r_send(d, b, hh):
            return remote(rout.at[b, half(hh)], rin.at[d, b, half(hh)],
                          rs_s.at[b, hh], rs_r.at[d, b, hh], ahead[d])

        lax.fori_loop(0, 2, rs, 0)

        @pl.when(t < 8)
        def _():
            k = t // 2
            chip = turn(z, k)
            odd = t % 2
            core = jnp.where(odd == 0, c, 1 - c)
            blk = block_of(chip, core)
            local(pre_ref.at[blk], preb, 0).wait()
            local(dy_ref, dyb.at[pl.ds(0, B)], 1).wait()

            def t1(n, _):
                cs = cols(n)
                g = lax.dot_general(dyb[pl.ds(0, B), :], wd[cs, :], NT, preferred_element_type=F32)
                hidden, slope = gelu_and_slope(preb[:, cs].astype(F32))
                hid[pl.ds(0, B), cs] = hidden.astype(BF16)
                dp[blk, cs] = (g * slope).astype(BF16)
                return 0

            lax.fori_loop(0, F // TILE, t1, 0)

            @pl.when(t < 7)
            def _():
                core = jnp.where(odd == 1, c, 1 - c)
                local(pre_ref.at[block_of(turn(z, (t + 1) // 2), core)], preb, 0).start()

            @pl.when(t == 0)
            def _():
                local(x_ref, pxb, 12).wait()
                local(pxb, xg.at[block_of(spot(1, z, z), c)], 12).start()

            @pl.when(odd == 1)
            def _():
                @pl.when(k == 0)
                def _():
                    local(pxb, xg.at[block_of(spot(1, z, z), c)], 12).wait()

                @pl.when(k > 0)
                def _():
                    px_send(chip, k - 1).wait_send()

                def px(n, _):
                    cs = cols(n)
                    g = lax.dot_general(dp[blk, :], wi[cs, :], NT, preferred_element_type=F32)
                    pxb[:, cs] = g.astype(BF16)
                    return 0

                lax.fori_loop(0, D // TILE, px, 0)
                settle()
                px_send(chip, k).start()

            def t2(m, _):
                ms = cols(m)
                acc[ms, :] += lax.dot_general(hid[:, ms], dyb[...], TN, preferred_element_type=F32)
                return 0

            lax.fori_loop(0, F // TILE, t2, 0)

        @pl.when(t == 2)
        def _():
            pv[...] = jnp.zeros(pv.shape, BF16)

            @pl.when(((z > 0) & (z < Z - 1)) | (c == 0))
            def _():
                sync(pv.at[pl.ds(0, mid)], came_o.at[pl.ds(early, mid)], 13)

            @pl.when((z > 0) & (z < Z - 1))
            def _():
                sync(pv.at[pl.ds(0, early)], came_o.at[pl.ds(0, early)], 13)

        @pl.when(t == 8)
        def _():
            for k in (2, 3):
                local(dp.at[chip_rows(turn(z, k))], dpre_o.at[pl.ds((k - 2) * 2 * B, 2 * B)], k).start()
            px_send(0, 3).wait_send()

            def flush(m, _):
                ms = cols(m)
                pxb[pl.ds(0, TILE), :] = acc[ms, :].astype(BF16)
                acc[ms, :] = jnp.zeros((TILE, D), F32)
                sync(pxb.at[pl.ds(0, TILE)], dwd_o.at[ms], 13)
                return 0

            lax.fori_loop(0, F // TILE, flush, 0)

        @pl.when((t >= 8) & (t < 12))
        def _():
            k = (t - 8) // 2
            chip = turn(z, k)
            core = jnp.where(t % 2 == 0, c, 1 - c)
            local(x_ref, dyb.at[pl.ds(0, B)], 1).wait()

            def t4(m, _):
                for i in (0, 1):
                    acc[cols(m), pl.ds(i * F, F)] += lax.dot_general(
                        dyb[pl.ds(0, B), cols(2 * m + i)], dp[block_of(chip, core), :], TN,
                        preferred_element_type=F32)
                return 0

            lax.fori_loop(0, D // (2 * TILE), t4, 0)
        return 0

    lax.fori_loop(0, 13, slot, 0)

    for k in (2, 3):
        local(dp.at[pl.ds(0, 2 * B)], dpre_o.at[pl.ds(0, 2 * B)], k).wait()
        for h in (0, 1):
            from_partner(1, turn(z, k), h).wait_recv()
    for chip in range(Z):
        for h in (0, 1):
            for a in (0, 1):
                to_partner(a, chip, h).wait_send()
            kept = ((z == 1) & (chip == 0)) | ((z == Z - 2) & (chip == Z - 1))

            @pl.when(kept & ((h == 0) | (c == 1)))
            def _():
                (mid_send if h else end_send)(0, chip).wait_send()

            @pl.when((z != chip) & jnp.logical_not(kept))
            def _():
                remote(rout.at[chip, half(h)], rin.at[0, chip, half(h)],
                       rs_s.at[chip, h], rs_r.at[0, chip, h], partner).wait_send()
    for d in (0, 1):
        @pl.when(place[d] == Z - 1)
        def _():
            end_send(d, z).wait_recv()

            @pl.when(c == 1)
            def _():
                mid_send(d, z).wait_recv()

        for s in range(Z - 1):
            @pl.when((place[d] < Z - 1) & (s <= place[d]))
            def _():
                for a in (0, 1):
                    for h in (0, 1):
                        line_send(d, a, s, h).wait_send()
    local(acc, part_o, 9).wait()


def line_step(x, dy, pre, w_in, w_down):
    B, D = dy.shape
    H = B // 2
    R, F = pre.shape
    PAD = -(-B // TILE) * TILE
    hbm = pl.BlockSpec(memory_space=pltpu.HBM)
    sds = jax.ShapeDtypeStruct
    dma = pltpu.SemaphoreType.DMA
    return pl.pallas_call(
        line_kernel,
        out_shape=[
            sds((R, D), BF16), sds((R, D), BF16), sds((R // 2, F), BF16), sds((F, D), BF16), sds((F, D), F32),
            sds((EARLY + MID, D), F32), sds((B - EARLY - MID, D), F32),
            sds((MID, D), BF16), sds((B - EARLY - MID, D), BF16), sds((EARLY + MID, D), BF16),
            sds((2, Z, B, D), BF16), sds((Z, B, D), BF16), sds((Z, B, D), BF16),
        ],
        in_specs=[hbm] * 5,
        out_specs=[hbm] * 13,
        scratch_shapes=[
            pltpu.VMEM((D, F), BF16), pltpu.VMEM((F, D), BF16), pltpu.VMEM((F, D), F32),
            pltpu.VMEM((R, F), BF16), pltpu.VMEM((PAD, D), BF16), pltpu.VMEM((B, F), BF16),
            pltpu.VMEM((PAD, F), BF16), pltpu.VMEM((B, D), BF16), pltpu.VMEM((H, D), BF16),
            pltpu.VMEM((2, H, D), BF16), pltpu.VMEM((H, D), BF16), pltpu.VMEM((H, D), F32),
            dma((2, 2, 3, 2)), dma((2, 2, 3, 2)), dma((2, Z, 2)), dma((2, Z, 2)),
            dma((Z,)), dma((Z,)), dma((Z, 2)), dma((2, Z, 2)), dma((14,)), pltpu.SemaphoreType.REGULAR,
        ],
        compiler_params=pltpu.CompilerParams(
            collective_id=0, has_side_effects=True, vmem_limit_bytes=62 * 1024 * 1024
        ),
        cost_estimate=pl.CostEstimate(flops=6 * R * D * F, bytes_accessed=12 * R * D, transcendentals=R * F),
    )(x, dy, pre, w_in, w_down)


def dw_kernel(a_ref, b_ref, part_ref, o_ref):
    rows, width = part_ref.shape[0], b_ref.shape[1]
    for i in (0, 1):
        band = pl.ds(i * rows, rows)
        g = lax.dot_general(a_ref[:, band], b_ref[...], TN, preferred_element_type=F32)
        o_ref[band, :] = (part_ref[:, pl.ds(i * width, width)] + g).astype(o_ref.dtype)


def finish_dw(x, d_pre, part):
    D = x.shape[1]
    R, F = d_pre.shape
    n = D // (2 * TILE)
    last = x.shape[0] // R - 1
    return pl.pallas_call(
        dw_kernel,
        grid=(n,),
        out_shape=jax.ShapeDtypeStruct((D, F), BF16),
        in_specs=[pl.BlockSpec((R, D // n), lambda i: (last, i)), pl.BlockSpec((R, F), lambda i: (0, 0)),
                  pl.BlockSpec((F // n, D), lambda i: (i, 0))],
        out_specs=pl.BlockSpec((D // n, F), lambda i: (i, 0)),
        compiler_params=pltpu.CompilerParams(vmem_limit_bytes=48 * 1024 * 1024),
        cost_estimate=pl.CostEstimate(flops=2 * R * D * F, bytes_accessed=2 * (R * D + R * F + 3 * D * F), transcendentals=0),
    )(x, d_pre, part)


def pass_kernel(w_ref, base_ref, came_ref, mid_ref, wo_ref, dx_ref):
    wo_ref[...] = w_ref[...]

    @pl.when(pl.program_id(0) == 0)
    def _():
        for first, count, more in ((0, EARLY, None), (EARLY, MID, mid_ref)):
            rows = pl.ds(first, count)
            total = base_ref[rows, :] + came_ref[rows, :].astype(F32)
            if more is not None:
                total = total + more[...].astype(F32)
            dx_ref[rows, :] = total.astype(dx_ref.dtype)


def pass_on(dw_down, base, came, mid, rows):
    F, D = dw_down.shape
    sds = jax.ShapeDtypeStruct
    down = pl.BlockSpec((F // 2, D), lambda i: (i, 0))
    strip = pl.BlockSpec((EARLY + MID, D), lambda i: (0, 0))
    return pl.pallas_call(
        pass_kernel,
        grid=(2,),
        out_shape=[sds((F, D), BF16), sds((rows, D), BF16)],
        in_specs=[down, strip, strip, pl.BlockSpec((MID, D), lambda i: (0, 0))],
        out_specs=[down, strip],
        compiler_params=pltpu.CompilerParams(vmem_limit_bytes=32 * 1024 * 1024),
        cost_estimate=pl.CostEstimate(flops=4 * F * D * 512, bytes_accessed=4 * F * D, transcendentals=0),
    )(dw_down, base, came, mid)


def solution(mesh):
    def body(x, dy, pre, w_in, w_down):
        xg, _, d_pre, dw_down, part, base, last_base, mid, last, came, _, _, _ = line_step(x, dy, pre, w_in, w_down)
        hops = [[(2 + c, c), (2 * Z - 4 + c, 2 * Z - 2 + c)] for c in (0, 1)]
        mid = lax.ppermute(mid, "tp", hops[0])
        last = lax.ppermute(last, "tp", hops[0] + hops[1])
        dw_in = finish_dw(xg, d_pre, part)
        dw_down, dx = pass_on(dw_down, base, came, mid, x.shape[0])
        dx = lax.dynamic_update_slice(dx, (last_base + last.astype(F32)).astype(BF16), (EARLY + MID, 0))
        return dx, dw_in, dw_down

    rows = P(("dp", "tp"), None)
    return jax.shard_map(
        body, mesh=mesh,
        in_specs=(rows, rows, P("dp", "tp"), P(None, "tp"), P("tp", None)),
        out_specs=(rows, P("dp", "tp"), rows),
        check_vma=False,
    )
```
